128 devices in a mesh: front: 4 (over y), row: 4 (over z_lo, core), col: 8 (over x, z_hi).
Axes of the slice: x: 4, y: 4, z: 4 (z_hi: 2, z_lo: 2; z = z_hi * 2 + z_lo), core: 2. Of those that a mesh axis runs over, the one named last changes fastest.
Arguments:
- pivot_block: bfloat16 [4, 1024, 1024], P('front'), may hold values from -6 to 6
- border: bfloat16 [4, 8192, 1024], P('front', 'row'), may hold values from -6 to 6
- contrib: bfloat16 [4, 8192, 8192], P('front', 'row', 'col'), may hold values from -6 to 6
- inverses: bfloat16 [4, 4, 256, 256], P('front'), may hold values from -0.0625 to 0.0625
- row_tiles: int32 [4, 64], replicated, may hold values from 0 to 79, as said below
- col_tiles: int32 [4, 64], replicated, may hold values from 0 to 79, as said below
- owner: int32 [80], replicated, may hold values from 0 to 79, as said below
- schur_init: bfloat16 [10240, 10240], P(('front', 'row'), 'col'), may hold values from -6 to 6
- block: bfloat16 [10240, 512], P('col'), may hold values from -0.0625 to 0.0625
Outputs:
- schur: float32 [10240, 10240], P(('front', 'row'), 'col')
- product: float32 [10240, 512], P(('front', 'row', 'col'))
The draws below stay inside these ranges and needn't reach their ends.
Inputs may be any that keep to these rules, and one draw needn't show every extreme that they name: owner is a permutation of 0 .. 79. For each front the 64 entries are distinct. With s = owner[row_tiles[f, i]], each front has exactly 4 entries in each group s // 5; among the 16 entries of one aligned block of a front at most 2 fall in one group, and that many in some block of every draw. For each front the 64 entries are distinct. With s = owner[col_tiles[f, j]], each front has exactly 8 entries in each group s // 10; among the 8 entries of one aligned block of a front at most 2 fall in one group, and that many in some block of every draw.
All inputs are finite; a program needn't handle non-finite values.
Results may differ from the reference program's by a relative error of at most 0.008.
Values may be sent and summed in bfloat16 or wider, within the bound.
A program may use at most 128 MiB of HBM per device.

```python
import jax
import jax.numpy as jnp

C = 8192
NB = 256
PANELS = 4
TILE = 128
SN = 10240
BW = 512
FRONTS = 4
P_SIZE = 1024
CT = 64
ST = 80
N_FRONT = 4
N_ROW = 4
N_COL = 8


def tile_layout(key, blocks, groups, per_group, used):
    total = groups * used
    base = total // (blocks * groups)
    flips = jax.random.randint(jax.random.fold_in(key, 1), (blocks // 2, groups // 2), -1, 2)
    flips = flips.at[0, 0].set(1)
    stepped = flips * base
    pattern = jnp.stack([jnp.stack([stepped, -stepped], -1), jnp.stack([-stepped, stepped], -1)], 1)
    counts = base + pattern.reshape(blocks, groups)
    group_keys = jax.random.split(jax.random.fold_in(key, 2), groups)
    chosen = jax.vmap(lambda single: jnp.sort(jax.random.permutation(single, per_group)[:used]))(group_keys)
    running = jnp.cumsum(counts, axis=0)
    holder = jnp.sum((running[:, :, None] <= jnp.arange(used)[None, None, :]).astype(jnp.int32), axis=0)
    shuffle = jax.random.permutation(jax.random.fold_in(key, 3), total)
    scores = holder.reshape(-1) * total + shuffle
    ordering = jnp.argsort(scores)
    slots = (jnp.arange(groups)[:, None] * per_group + chosen).reshape(-1)
    return slots[ordering].astype(jnp.int32)


def draw_owner(key, part):
    return jax.random.permutation(jax.random.fold_in(key, 7), ST).astype(jnp.int32)


def draw_row_tiles(key, part):
    inverse_map = jnp.argsort(draw_owner(key, part)).astype(jnp.int32)
    groups = N_FRONT * N_ROW
    lists = [inverse_map[tile_layout(jax.random.fold_in(key, 100 + front_index), N_ROW, groups, ST // groups, CT // groups)] for front_index in range(FRONTS)]
    return jnp.stack(lists).astype(jnp.int32)


def draw_col_tiles(key, part):
    inverse_map = jnp.argsort(draw_owner(key, part)).astype(jnp.int32)
    lists = [inverse_map[tile_layout(jax.random.fold_in(key, 200 + front_index), N_COL, N_COL, ST // N_COL, CT // N_COL)] for front_index in range(FRONTS)]
    return jnp.stack(lists).astype(jnp.int32)


def block_scale(key, shape, shards, smallest, top_value):
    factor_of, own = 1.0, jax.random.fold_in(key, 6)
    for position, parts in shards:
        draws = jnp.exp(jax.random.uniform(jax.random.fold_in(own, position), (parts,), jnp.float32, smallest / len(shards), top_value / len(shards)))
        factor_of = factor_of * jnp.repeat(draws, shape[position] // parts).reshape([-1 if axis == position else 1 for axis in range(len(shape))])
    return factor_of


def noise(key, dims, scale, most, cuts=(), dtype=jnp.bfloat16):
    level = block_scale(key, dims, cuts, -0.22, 0.18) if cuts else 1.0
    entries = jax.random.normal(key, dims, jnp.float32) * scale * level
    return jnp.minimum(jnp.maximum(entries, -most), most).astype(dtype)


def setup_inputs(seed: int = 0) -> dict:
    seeds = jax.random.split(jax.random.key(seed), 10)
    pivot_block = noise(seeds[0], (FRONTS, P_SIZE, P_SIZE), 1.0, 6.0, ((0, 4),))
    border = noise(seeds[1], (FRONTS, C, P_SIZE), 1.0, 6.0, ((0, 4), (1, 4)))
    contrib = noise(seeds[2], (FRONTS, C, C), 1.0, 6.0, ((0, 4), (1, 4), (2, 8)))
    inverses = noise(seeds[3], (FRONTS, PANELS, NB, NB), (32 * NB) ** -0.5, 0.0625, ((0, 4),))
    row_tiles = draw_row_tiles(jax.random.fold_in(seeds[9], 71), 0)
    col_tiles = draw_col_tiles(jax.random.fold_in(seeds[9], 71), 0)
    owner = draw_owner(jax.random.fold_in(seeds[9], 71), 0)
    schur_init = noise(seeds[7], (SN, SN), 1.0, 6.0, ((0, 16), (1, 8)))
    block = noise(seeds[8], (SN, BW), SN ** -0.5, 0.0625, ((0, 8),))
    return {"pivot_block": pivot_block, "border": border, "contrib": contrib, "inverses": inverses, "row_tiles": row_tiles, "col_tiles": col_tiles, "owner": owner, "schur_init": schur_init, "block": block}


def eliminate(pivot, rows, inverse_set):
    pivot_now = pivot.astype(jnp.float32)
    rows_now = rows.astype(jnp.float32)
    leaves = []
    for panel_index in range(PANELS):
        start = panel_index * NB
        left = pivot_now[:, start:start + NB].astype(jnp.bfloat16)
        below = jnp.arange(P_SIZE)[:, None] >= start + NB
        lower = jnp.where(below, jnp.dot(left, inverse_set[panel_index], preferred_element_type=jnp.float32), 0.0).astype(jnp.bfloat16)
        side = jnp.dot(rows_now[:, start:start + NB].astype(jnp.bfloat16), inverse_set[panel_index], preferred_element_type=jnp.float32).astype(jnp.bfloat16)
        pivot_now = pivot_now - jnp.dot(lower, lower.T, preferred_element_type=jnp.float32)
        rows_now = rows_now - jnp.dot(side, lower.T, preferred_element_type=jnp.float32)
        leaves.append(side)
    return jnp.concatenate(leaves, axis=1)


def reference(pivot_block, border, contrib, inverses, row_tiles, col_tiles, owner, schur_init, block):
    slot_rows = owner[row_tiles]
    slot_cols = owner[col_tiles]
    tiled = jnp.zeros((ST, ST, TILE, TILE), jnp.float32)
    for front_index in range(FRONTS):
        factor = eliminate(pivot_block[front_index], border[front_index], inverses[front_index])
        update = (contrib[front_index].astype(jnp.float32) - jnp.dot(factor, factor.T, preferred_element_type=jnp.float32)).astype(jnp.bfloat16)
        pieces = update.astype(jnp.float32).reshape(CT, TILE, CT, TILE).transpose(0, 2, 1, 3)
        tiled = tiled.at[slot_rows[front_index][:, None], slot_cols[front_index][None, :]].add(pieces)
    schur = schur_init.astype(jnp.float32) + tiled.transpose(0, 2, 1, 3).reshape(SN, SN)
    product = jnp.dot(schur.astype(jnp.bfloat16), block, preferred_element_type=jnp.float32)
    return (schur, product)
```

```python
import functools

import jax
import jax.numpy as jnp
from jax import lax
from jax.experimental import pallas as pl
from jax.experimental.pallas import tpu as pltpu
from jax.sharding import PartitionSpec as P

TILE = 128
MESH = pl.DeviceIdType.MESH
F32 = jnp.float32
BF16 = jnp.bfloat16


def nt(a, b):
    return lax.dot_general(a, b, (((1,), (1,)), ((), ())), preferred_element_type=F32)


def split_levels(src_c, src_r, dst_c, dst_r, squarings):
    n = src_c.shape[0]
    at_c = lax.broadcasted_iota(jnp.int32, (n, n), 0).astype(F32)
    at_r = lax.broadcasted_iota(jnp.int32, (n, n), 1).astype(F32)
    color_c = jnp.zeros((n, 1), F32)
    color_r = jnp.zeros((1, n), F32)

    def partners(node_c, node_r):
        same = jnp.where((node_c == node_r) & (color_c == color_r), 1.0, 0.0)
        rank_c = jnp.sum(jnp.where(at_r < at_c, same, 0.0), axis=1, keepdims=True)
        rank_r = jnp.sum(jnp.where(at_c < at_r, same, 0.0), axis=0, keepdims=True)
        pair = (jnp.floor(rank_c * 0.5) == jnp.floor(rank_r * 0.5)) & (at_c != at_r)
        return jnp.where(pair, same, 0.0)

    for count in squarings:
        by_src = partners(src_c, src_r)
        by_dst = partners(dst_c, dst_r)
        reach = jnp.dot(by_src.astype(BF16), by_dst.astype(BF16), preferred_element_type=F32)
        reach = jnp.where(at_c == at_r, 1.0, reach)
        for _ in range(count):
            half = reach.astype(BF16)
            reach = jnp.where(jnp.dot(half, half, preferred_element_type=F32) > 0.5, 1.0, 0.0)
        far = float(n)
        label_c = jnp.min(jnp.where(reach > 0.5, at_r, far), axis=1, keepdims=True)
        label_r = jnp.min(jnp.where(reach > 0.5, at_c, far), axis=0, keepdims=True)
        other_c = jnp.sum(by_src * label_r, axis=1, keepdims=True)
        other_r = jnp.sum(by_src * label_c, axis=0, keepdims=True)
        color_c = color_c * 2.0 + jnp.where(label_c > other_c, 1.0, 0.0)
        color_r = color_r * 2.0 + jnp.where(label_r > other_r, 1.0, 0.0)
    return color_c


def div(x, by):
    return jnp.floor((x + 0.5) * (1.0 / by))


def routing(rows_c, rows_r, cols_c, cols_r, owner_r, owner_c, front, row, col):
    n = rows_c.shape[0]
    per = n // 4
    slots = owner_r.shape[1]
    lane = lax.broadcasted_iota(jnp.int32, (n, slots), 1)
    sub = lax.broadcasted_iota(jnp.int32, (slots, n), 0)
    own_r = owner_r.astype(F32)
    own_c = owner_c.astype(F32)

    def slot_c(ids):
        return jnp.sum(jnp.where(ids == lane, own_r, 0.0), axis=1, keepdims=True)

    def slot_r(ids):
        return jnp.sum(jnp.where(ids == sub, own_c, 0.0), axis=0, keepdims=True)

    e_c = lax.broadcasted_iota(jnp.int32, (n, 1), 0).astype(F32)
    e_r = lax.broadcasted_iota(jnp.int32, (1, n), 1).astype(F32)
    f_c, f_r = div(e_c, per), div(e_r, per)
    i_c = e_c - f_c * per
    rs_c, rs_r, cs_c, cs_r = slot_c(rows_c), slot_r(rows_r), slot_c(cols_c), slot_r(cols_r)
    g_c, g_r, h_c, h_r = div(rs_c, 5), div(rs_r, 5), div(cs_c, 10), div(cs_r, 10)
    a_c, b_c = rs_c - g_c * 5, cs_c - h_c * 10
    mr = split_levels(div(e_c, 4), div(e_r, 4), f_c * 16 + g_c, f_r * 16 + g_r, (5, 4))
    mc = split_levels(div(e_c, 8), div(e_r, 8), f_c * 8 + h_c, f_r * 8 + h_r, (5, 4, 3))
    front, row, col = front.astype(F32), row.astype(F32), col.astype(F32)
    mine = f_c == front
    q = lax.broadcasted_iota(jnp.int32, (n, TILE), 1).astype(F32)

    def table(mask, value):
        return jnp.sum(jnp.where(mask, value, 0.0), axis=0, keepdims=True)

    in_row = i_c - div(i_c, 16) * 16
    chunk = div(in_row, 4)
    t0 = table(mine & (div(i_c, 16) == row) & (mr * 4 + chunk == q), in_row)
    block = div(i_c, 8)
    t1 = table(mine & (block == col) & (mc == q), i_c - block * 8)
    t2 = table(mine & (mr == row) & (g_c == q), div(i_c, 4))
    t3 = table(mine & (mc == col) & (h_c == q), block)
    t4 = table((g_c == front * 4 + row) & (f_c * 5 + a_c == q), mr + 1.0)
    t5 = table((h_c == col) & (f_c * 10 + b_c == q), mc + 1.0)
    zero = jnp.zeros_like(t0)
    return jnp.concatenate([t0, t1, t2, t3, t4, t5, zero, zero], axis=0).astype(jnp.int32)


def routing_kernel(rows_c, rows_r, cols_c, cols_r, owner_r, owner_c, out):
    out[...] = routing(
        rows_c[...], rows_r[...], cols_c[...], cols_r[...], owner_r[...], owner_c[...],
        lax.axis_index("front"), lax.axis_index("row"), lax.axis_index("col"),
    )


def route_tables(row_tiles, col_tiles, owner):
    n, slots = row_tiles.size, owner.size
    return pl.pallas_call(
        routing_kernel,
        out_shape=jax.ShapeDtypeStruct((8, TILE), jnp.int32),
        name="route_tables",
    )(
        row_tiles.reshape(n, 1), row_tiles.reshape(1, n), col_tiles.reshape(n, 1), col_tiles.reshape(1, n),
        owner.reshape(1, slots), owner.reshape(slots, 1),
    )


def position():
    front, row, col = lax.axis_index("front"), lax.axis_index("row"), lax.axis_index("col")
    return front, row // 2, row % 2, col // 2, col % 2


def device(front, z, core, x):
    return (front, (z % 2) * 2 + core, x * 2 + z // 2)


def eliminate_rows(block, lower, inverse_set):
    parts = []
    for k in range(4):
        now = block[:, k * 256 : (k + 1) * 256].astype(F32)
        for j in range(k):
            now = now - nt(parts[j], lower[k * 256 : (k + 1) * 256, j * 256 : (j + 1) * 256])
        parts.append(
            jnp.dot(now.astype(BF16), inverse_set[k], preferred_element_type=F32).astype(BF16)
        )
    return parts


def update_kernel(
    tab, pivot, border, contrib, inverse_set, out,
    rows_v, theirs, theirs_p, contrib_v, lower, out_v, lsem, osem, ssem, rsem,
):
    front, z_lo, core, x, z_hi = position()
    z = z_hi * 2 + z_lo
    up, down = (z + 1) % 4, (z + 3) % 4
    on_source_chip = z_lo == x // 2
    is_source = on_source_chip & (core == x % 2)
    sibling = device(front, z, 1 - core, x)
    barrier = pltpu.get_barrier_semaphore()
    for peer in (sibling, *(device(front, zz, k, x) for zz in (up, down) for k in (0, 1))):
        pl.semaphore_signal(barrier, inc=1, device_id=peer, device_id_type=MESH)
    load_lower = pltpu.make_async_copy(pivot.at[0], lower, lsem.at[0])
    load_rows = pltpu.make_async_copy(border, rows_v, lsem.at[1])
    load_contrib = [
        pltpu.make_async_copy(
            contrib.at[:, :, j * TILE : (j + 1) * TILE], contrib_v.at[j], lsem.at[2 + j]
        )
        for j in range(8)
    ]
    load_lower.start()
    load_rows.start()
    for copy in load_contrib:
        copy.start()
    pl.semaphore_wait(barrier, 5)

    def push(src, quarter, sem, peer):
        return pltpu.make_async_remote_copy(
            src_ref=src, dst_ref=theirs.at[pl.ds(2 * quarter, 2)], send_sem=ssem.at[sem], recv_sem=rsem.at[quarter],
            device_id=peer, device_id_type=MESH,
        )

    def quarter_of(half, q):
        return border.at[pl.ds(half * 8 + q * 2, 2)]

    def source_sends():
        sends = []
        for q in (0, 1):
            sends.append(push(quarter_of(up // 2, q), q, q, device(front, up, q, x)))
            sends.append(push(quarter_of(down // 2, 2 + q), 2 + q, 2 + q, device(front, down, q, x)))
        for q in range(4):
            sends.append(push(quarter_of(z_hi, q), q, 4 + q, sibling))
        return sends

    def own_quarters():
        return [pltpu.make_async_copy(quarter_of(z_hi, q), theirs.at[pl.ds(2 * q, 2)], lsem.at[11 + q]) for q in range(4)]

    @pl.when(is_source)
    def _():
        for copy in source_sends():
            copy.start()
        for copy in own_quarters():
            copy.start()

    load_lower.wait()
    for k in range(3):
        low = (k + 1) * 256
        now = lower[low:, k * 256 : (k + 1) * 256].astype(F32)
        for j in range(k):
            now = now - nt(
                lower[low:, j * 256 : (j + 1) * 256], lower[k * 256 : low, j * 256 : (j + 1) * 256]
            )
        lower[low:, k * 256 : (k + 1) * 256] = jnp.dot(
            now.astype(BF16), inverse_set[0, k], preferred_element_type=F32
        ).astype(BF16)
    load_rows.wait()

    def own_block(i, _):
        rows = pl.ds(i * 4, 4)
        parts = eliminate_rows(rows_v[rows].reshape(512, 1024), lower, inverse_set.at[0])
        for k in range(4):
            rows_v[rows, :, k * 256 : (k + 1) * 256] = parts[k].reshape(4, TILE, 256)
        return 0

    lax.fori_loop(0, 4, own_block, 0)

    def wait_quarter(q):
        push(theirs.at[pl.ds(2 * q, 2)], q, 0, sibling).wait_recv()

    def forwards():
        return [
            push(theirs.at[pl.ds(2 * q, 2)], q, i, sibling) for i, q in enumerate((core, 2 + core))
        ]

    @pl.when(is_source)
    def _():
        for copy in own_quarters():
            copy.wait()

    @pl.when(jnp.logical_not(on_source_chip))
    def _():
        first, second = forwards()
        wait_quarter(core)
        first.start()
        wait_quarter(2 + core)
        second.start()
        wait_quarter(1 - core)
        wait_quarter(3 - core)

    @pl.when(on_source_chip & jnp.logical_not(is_source))
    def _():
        for q in range(4):
            wait_quarter(q)

    @pl.when(is_source)
    def _():
        for copy in source_sends():
            copy.wait_send()

    @pl.when(jnp.logical_not(on_source_chip))
    def _():
        for copy in forwards():
            copy.wait_send()

    def their_block(i, _):
        rows = pl.ds(i * 4, 4)
        parts = eliminate_rows(theirs[rows].reshape(512, 1024), lower, inverse_set.at[0])
        for k in range(4):
            theirs[rows, :, k * 256 : (k + 1) * 256] = parts[k].reshape(4, TILE, 256)
        return 0

    lax.fori_loop(0, 2, their_block, 0)
    for m in range(8):
        theirs_p[m] = theirs[tab[1, m]]
    for copy in load_contrib:
        copy.wait()

    def packed(mr):
        return pltpu.make_async_copy(out_v.at[mr], out.at[mr], osem.at[mr])

    for mr in range(4):
        left = jnp.concatenate([rows_v[tab[0, mr * 4 + k]] for k in range(4)], axis=0)

        def two_cols(n, _):
            product = nt(left, theirs_p[pl.ds(n * 2, 2)].reshape(256, 1024))
            for t in range(2):
                for k in range(4):
                    tile = contrib_v[tab[1, 2 * n + t], tab[0, mr * 4 + k]].astype(F32)
                    part = product[k * TILE : (k + 1) * TILE, t * TILE : (t + 1) * TILE]
                    out_v[mr, 2 * n + t, k] = (tile - part).astype(BF16)
            return 0

        lax.fori_loop(0, 4, two_cols, 0)
        packed(mr).start()
    for mr in range(4):
        packed(mr).wait()


def packed_update(tables, pivot, border, contrib, inverse_set):
    vmem = pl.BlockSpec(memory_space=pltpu.VMEM)
    hbm = pl.BlockSpec(memory_space=pl.ANY)
    return pl.pallas_call(
        update_kernel,
        out_shape=jax.ShapeDtypeStruct((4, 8, 4, TILE, TILE), BF16),
        in_specs=[pl.BlockSpec(memory_space=pltpu.SMEM), hbm, hbm, hbm, vmem],
        out_specs=hbm,
        scratch_shapes=[
            pltpu.VMEM((16, TILE, 1024), BF16),
            pltpu.VMEM((8, TILE, 1024), BF16),
            pltpu.VMEM((8, TILE, 1024), BF16),
            pltpu.VMEM((8, 16, TILE, TILE), BF16),
            pltpu.VMEM((1024, 1024), BF16),
            pltpu.VMEM((4, 8, 4, TILE, TILE), BF16),
            pltpu.SemaphoreType.DMA((15,)),
            pltpu.SemaphoreType.DMA((4,)),
            pltpu.SemaphoreType.DMA((8,)),
            pltpu.SemaphoreType.DMA((4,)),
        ],
        compiler_params=pltpu.CompilerParams(
            collective_id=0, has_side_effects=True, vmem_limit_bytes=60 << 20
        ),
        name="packed_update",
    )(tables, pivot, border.reshape(16, TILE, 1024), contrib.reshape(16, TILE, 1024), inverse_set)


def reorder_kernel(tab, arrived, out):
    for h in range(8):
        out[0, h] = arrived[0, tab[3, h], 0]


def reorder(tables, arrived):
    return pl.pallas_call(
        reorder_kernel,
        out_shape=jax.ShapeDtypeStruct((16, 8, TILE, TILE), BF16),
        grid_spec=pltpu.PrefetchScalarGridSpec(
            num_scalar_prefetch=1,
            grid=(16,),
            in_specs=[
                pl.BlockSpec(
                    (1, 8, 1, TILE, TILE), lambda g, tab: (tab[2, g] // 4, 0, tab[2, g] % 4, 0, 0)
                )
            ],
            out_specs=pl.BlockSpec((1, 8, TILE, TILE), lambda g, tab: (g, 0, 0, 0)),
        ),
        name="reorder",
    )(tables, arrived.reshape(4, 8, 4, TILE, TILE))


def assemble_kernel(tab, t0, t1, t2, t3, init, vectors, schur, partial):
    a = pl.program_id(0)
    tiles = (t0, t1, t2, t3)
    for b in range(10):
        cols = slice(b * TILE, (b + 1) * TILE)
        total = init[:, cols].astype(F32)
        for f in range(4):
            m = tab[5, f * 10 + b]
            there = (m > 0) & (tab[4, f * 5 + a] > 0)
            tile = tiles[f][0, 0, jnp.maximum(m - 1, 0)].astype(F32)
            total = total + jnp.where(there, tile, 0.0)
        schur[:, cols] = total
    partial[...] = jnp.dot(
        schur[...].astype(BF16), vectors[...], preferred_element_type=F32
    ).astype(partial.dtype)


def assemble(tables, arrived, init, vectors):
    def pick(f):
        return pl.BlockSpec(
            (1, 1, 8, TILE, TILE), lambda a, tab: (f, jnp.maximum(tab[4, f * 5 + a] - 1, 0), 0, 0, 0)
        )

    arrived = arrived.reshape(4, 4, 8, TILE, TILE)
    rows, cols = init.shape
    wide = vectors.shape[1]
    return pl.pallas_call(
        assemble_kernel,
        out_shape=(
            jax.ShapeDtypeStruct((rows, cols), F32),
            jax.ShapeDtypeStruct((rows, wide), BF16),
        ),
        grid_spec=pltpu.PrefetchScalarGridSpec(
            num_scalar_prefetch=1,
            grid=(rows // TILE,),
            in_specs=[
                *(pick(f) for f in range(4)),
                pl.BlockSpec((TILE, cols), lambda a, tab: (a, 0)),
                pl.BlockSpec((cols, wide), lambda a, tab: (0, 0)),
            ],
            out_specs=(
                pl.BlockSpec((TILE, cols), lambda a, tab: (a, 0)),
                pl.BlockSpec((TILE, wide), lambda a, tab: (a, 0)),
            ),
        ),
        name="assemble",
    )(tables, arrived, arrived, arrived, arrived, init, vectors)


def shards(pivot_block, border, contrib, inverses, row_tiles, col_tiles, owner, schur_init, block):
    tables = route_tables(row_tiles, col_tiles, owner)
    packed = packed_update(tables, pivot_block, border, contrib, inverses)
    spread = lax.all_to_all(
        packed.reshape(32, 4, TILE, TILE), ("row", "col"), split_axis=0, concat_axis=0, tiled=True
    )
    ordered = reorder(tables, spread)
    arrived = lax.all_to_all(
        ordered.reshape(128, TILE, TILE), ("front", "row", "col"), split_axis=0, concat_axis=0, tiled=True
    )
    schur, partial = assemble(tables, arrived, schur_init, block)
    parts = lax.all_to_all(
        partial.reshape(8, 80, 512), "col", split_axis=0, concat_axis=0, tiled=True
    )
    product = parts.astype(F32).sum(axis=0)
    return schur, product


def solution(mesh):
    in_specs = (
        P("front", None, None),
        P("front", "row", None),
        P("front", "row", "col"),
        P("front", None, None, None),
        P(),
        P(),
        P(),
        P(("front", "row"), "col"),
        P("col", None),
    )
    out_specs = (P(("front", "row"), "col"), P(("front", "row", "col"), None))
    return jax.shard_map(shards, mesh=mesh, in_specs=in_specs, out_specs=out_specs, check_vma=False)
```

```python
import functools

import jax
import jax.numpy as jnp
from jax import lax
from jax.experimental import pallas as pl
from jax.experimental.pallas import tpu as pltpu
from jax.sharding import PartitionSpec as P

TILE = 128
MESH = pl.DeviceIdType.MESH
F32 = jnp.float32
BF16 = jnp.bfloat16


def nt(a, b):
    return lax.dot_general(a, b, (((1,), (1,)), ((), ())), preferred_element_type=F32)


def split_levels(src_c, src_r, dst_c, dst_r, squarings):
    n = src_c.shape[0]
    at_c = lax.broadcasted_iota(jnp.int32, (n, n), 0).astype(F32)
    at_r = lax.broadcasted_iota(jnp.int32, (n, n), 1).astype(F32)
    color_c = jnp.zeros((n, 1), F32)
    color_r = jnp.zeros((1, n), F32)

    def partners(node_c, node_r):
        same = jnp.where((node_c == node_r) & (color_c == color_r), 1.0, 0.0)
        rank_c = jnp.sum(jnp.where(at_r < at_c, same, 0.0), axis=1, keepdims=True)
        rank_r = jnp.sum(jnp.where(at_c < at_r, same, 0.0), axis=0, keepdims=True)
        pair = (jnp.floor(rank_c * 0.5) == jnp.floor(rank_r * 0.5)) & (at_c != at_r)
        return jnp.where(pair, same, 0.0)

    for count in squarings:
        by_src = partners(src_c, src_r)
        by_dst = partners(dst_c, dst_r)
        reach = jnp.dot(by_src.astype(BF16), by_dst.astype(BF16), preferred_element_type=F32)
        reach = jnp.where(at_c == at_r, 1.0, reach)
        for _ in range(count):
            half = reach.astype(BF16)
            reach = jnp.where(jnp.dot(half, half, preferred_element_type=F32) > 0.5, 1.0, 0.0)
        far = float(n)
        label_c = jnp.min(jnp.where(reach > 0.5, at_r, far), axis=1, keepdims=True)
        label_r = jnp.min(jnp.where(reach > 0.5, at_c, far), axis=0, keepdims=True)
        other_c = jnp.sum(by_src * label_r, axis=1, keepdims=True)
        other_r = jnp.sum(by_src * label_c, axis=0, keepdims=True)
        color_c = color_c * 2.0 + jnp.where(label_c > other_c, 1.0, 0.0)
        color_r = color_r * 2.0 + jnp.where(label_r > other_r, 1.0, 0.0)
    return color_c


def div(x, by):
    return jnp.floor((x + 0.5) * (1.0 / by))


def routing(rows_c, rows_r, cols_c, cols_r, owner_r, owner_c, front, row, col):
    n = rows_c.shape[0]
    per = n // 4
    slots = owner_r.shape[1]
    lane = lax.broadcasted_iota(jnp.int32, (n, slots), 1)
    sub = lax.broadcasted_iota(jnp.int32, (slots, n), 0)
    own_r = owner_r.astype(F32)
    own_c = owner_c.astype(F32)

    def slot_c(ids):
        return jnp.sum(jnp.where(ids == lane, own_r, 0.0), axis=1, keepdims=True)

    def slot_r(ids):
        return jnp.sum(jnp.where(ids == sub, own_c, 0.0), axis=0, keepdims=True)

    e_c = lax.broadcasted_iota(jnp.int32, (n, 1), 0).astype(F32)
    e_r = lax.broadcasted_iota(jnp.int32, (1, n), 1).astype(F32)
    f_c, f_r = div(e_c, per), div(e_r, per)
    i_c = e_c - f_c * per
    rs_c, rs_r, cs_c, cs_r = slot_c(rows_c), slot_r(rows_r), slot_c(cols_c), slot_r(cols_r)
    g_c, g_r, h_c, h_r = div(rs_c, 5), div(rs_r, 5), div(cs_c, 10), div(cs_r, 10)
    a_c, b_c = rs_c - g_c * 5, cs_c - h_c * 10
    mr = split_levels(div(e_c, 4), div(e_r, 4), f_c * 16 + g_c, f_r * 16 + g_r, (5, 4))
    mc = split_levels(div(e_c, 8), div(e_r, 8), f_c * 8 + h_c, f_r * 8 + h_r, (5, 4, 3))
    front, row, col = front.astype(F32), row.astype(F32), col.astype(F32)
    mine = f_c == front
    q = lax.broadcasted_iota(jnp.int32, (n, TILE), 1).astype(F32)

    def table(mask, value):
        return jnp.sum(jnp.where(mask, value, 0.0), axis=0, keepdims=True)

    in_row = i_c - div(i_c, 16) * 16
    chunk = div(in_row, 4)
    t0 = table(mine & (div(i_c, 16) == row) & (mr * 4 + chunk == q), in_row)
    block = div(i_c, 8)
    t1 = table(mine & (block == col) & (mc == q), i_c - block * 8)
    at_row = mine & (mr == row) & (g_c == q)
    t2 = table(at_row, div(i_c, 16) * 8)
    t3 = table(mine & (mc == col) & (h_c == q), block)
    t6 = table(at_row, chunk)
    t4 = table((g_c == front * 4 + row) & (f_c * 5 + a_c == q), mr + 1.0)
    t5 = table((h_c == col) & (f_c * 10 + b_c == q), mc + 1.0)
    zero = jnp.zeros_like(t0)
    return jnp.concatenate([t0, t1, t2, t3, t4, t5, t6, zero], axis=0).astype(jnp.int32)


def both_ways(ids):
    fronts, per = ids.shape
    n = fronts * per
    spread = jnp.where(
        lax.broadcasted_iota(jnp.int32, (per, n), 0) == lax.broadcasted_iota(jnp.int32, (per, n), 1) % per, 1.0, 0.0
    )
    wide = jnp.dot(ids.astype(F32).astype(BF16), spread.astype(BF16), preferred_element_type=F32)
    here = lax.broadcasted_iota(jnp.int32, (fronts, n), 0) == lax.broadcasted_iota(jnp.int32, (fronts, n), 1) // per
    flat = jnp.sum(jnp.where(here, wide, 0.0), axis=0, keepdims=True)
    return turned(flat).astype(jnp.int32), flat.astype(jnp.int32)


def turned(flat):
    n = flat.shape[1]
    eye = lax.broadcasted_iota(jnp.int32, (n, n), 0) == lax.broadcasted_iota(jnp.int32, (n, n), 1)
    return jnp.sum(jnp.where(eye, flat, 0.0), axis=1, keepdims=True)


def position():
    front, row, col = lax.axis_index("front"), lax.axis_index("row"), lax.axis_index("col")
    return front, row // 2, row % 2, col // 2, col % 2


def device(front, z, core, x):
    return (front, (z % 2) * 2 + core, x * 2 + z // 2)


def eliminate_rows(block, lower, inverse_set):
    parts = []
    for k in range(4):
        now = block[:, k * 256 : (k + 1) * 256].astype(F32)
        for j in range(k):
            now = now - nt(parts[j], lower[k * 256 : (k + 1) * 256, j * 256 : (j + 1) * 256])
        parts.append(
            jnp.dot(now.astype(BF16), inverse_set[k], preferred_element_type=F32).astype(BF16)
        )
    return parts


def eliminate_kernel(
    row_tiles, col_tiles, owner, pivot, border, inverse_set, tab, own_out, theirs_out,
    rows_v, theirs, lower, lsem, osem, ssem, rsem,
):
    front, z_lo, core, x, z_hi = position()
    z = z_hi * 2 + z_lo
    up, down = (z + 1) % 4, (z + 3) % 4
    on_source_chip = z_lo == x // 2
    is_source = on_source_chip & (core == x % 2)
    sibling = device(front, z, 1 - core, x)
    barrier = pltpu.get_barrier_semaphore()
    for peer in (sibling, *(device(front, zz, k, x) for zz in (up, down) for k in (0, 1))):
        pl.semaphore_signal(barrier, inc=1, device_id=peer, device_id_type=MESH)
    load_lower = pltpu.make_async_copy(pivot.at[0], lower, lsem.at[0])
    load_rows = pltpu.make_async_copy(border, rows_v, lsem.at[1])
    load_lower.start()
    load_rows.start()
    pl.semaphore_wait(barrier, 5)

    def push(src, quarter, sem, peer):
        return pltpu.make_async_remote_copy(
            src_ref=src, dst_ref=theirs.at[pl.ds(2 * quarter, 2)], send_sem=ssem.at[sem],
            recv_sem=rsem.at[quarter], device_id=peer, device_id_type=MESH,
        )

    def quarter_of(half, q):
        return border.at[pl.ds(half * 8 + q * 2, 2)]

    def source_sends():
        sends = []
        for q in (0, 1):
            sends.append(push(quarter_of(up // 2, q), q, q, device(front, up, q, x)))
            sends.append(push(quarter_of(down // 2, 2 + q), 2 + q, 2 + q, device(front, down, q, x)))
        for q in range(4):
            sends.append(push(quarter_of(z_hi, q), q, 4 + q, sibling))
        return sends

    def own_quarters():
        return [
            pltpu.make_async_copy(quarter_of(z_hi, q), theirs.at[pl.ds(2 * q, 2)], lsem.at[2 + q])
            for q in range(4)
        ]

    @pl.when(is_source)
    def _():
        for copy in source_sends():
            copy.start()
        for copy in own_quarters():
            copy.start()

    load_lower.wait()
    for k in range(3):
        low = (k + 1) * 256
        now = lower[low:, k * 256 : (k + 1) * 256].astype(F32)
        for j in range(k):
            now = now - nt(
                lower[low:, j * 256 : (j + 1) * 256], lower[k * 256 : low, j * 256 : (j + 1) * 256]
            )
        lower[low:, k * 256 : (k + 1) * 256] = jnp.dot(
            now.astype(BF16), inverse_set[0, k], preferred_element_type=F32
        ).astype(BF16)
    load_rows.wait()

    def block_of(buffer, target, base):
        def step(i, _):
            rows = pl.ds(i * 4, 4)
            parts = eliminate_rows(buffer[rows].reshape(512, 1024), lower, inverse_set.at[0])
            for k in range(4):
                buffer[rows, :, k * 256 : (k + 1) * 256] = parts[k].reshape(4, TILE, 256)
            pltpu.make_async_copy(buffer.at[rows], target.at[rows], osem.at[base + i]).start()
            return 0

        return step

    lax.fori_loop(0, 4, block_of(rows_v, own_out, 0), 0)
    rows_c, rows_r = both_ways(row_tiles[...])
    cols_c, cols_r = both_ways(col_tiles[...])
    tab[...] = routing(
        rows_c, rows_r, cols_c, cols_r, owner[...], turned(owner[...].astype(F32)),
        front, lax.axis_index("row"), lax.axis_index("col"),
    )

    def wait_quarter(q):
        push(theirs.at[pl.ds(2 * q, 2)], q, 0, sibling).wait_recv()

    def forwards():
        return [
            push(theirs.at[pl.ds(2 * q, 2)], q, i, sibling) for i, q in enumerate((core, 2 + core))
        ]

    @pl.when(is_source)
    def _():
        for copy in own_quarters():
            copy.wait()

    @pl.when(jnp.logical_not(on_source_chip))
    def _():
        first, second = forwards()
        wait_quarter(core)
        first.start()
        wait_quarter(2 + core)
        second.start()
        wait_quarter(1 - core)
        wait_quarter(3 - core)

    @pl.when(on_source_chip & jnp.logical_not(is_source))
    def _():
        for q in range(4):
            wait_quarter(q)

    @pl.when(is_source)
    def _():
        for copy in source_sends():
            copy.wait_send()

    @pl.when(jnp.logical_not(on_source_chip))
    def _():
        for copy in forwards():
            copy.wait_send()

    lax.fori_loop(0, 2, block_of(theirs, theirs_out, 4), 0)
    for i in range(4):
        rows = pl.ds(i * 4, 4)
        pltpu.make_async_copy(rows_v.at[rows], own_out.at[rows], osem.at[i]).wait()
    for i in range(2):
        rows = pl.ds(i * 4, 4)
        pltpu.make_async_copy(theirs.at[rows], theirs_out.at[rows], osem.at[4 + i]).wait()


def eliminate(row_tiles, col_tiles, owner, pivot, border, inverse_set):
    vmem = pl.BlockSpec(memory_space=pltpu.VMEM)
    hbm = pl.BlockSpec(memory_space=pl.ANY)
    return pl.pallas_call(
        eliminate_kernel,
        out_shape=(
            jax.ShapeDtypeStruct((8, TILE), jnp.int32),
            jax.ShapeDtypeStruct((16, TILE, 1024), BF16),
            jax.ShapeDtypeStruct((8, TILE, 1024), BF16),
        ),
        in_specs=[vmem, vmem, vmem, hbm, hbm, vmem],
        out_specs=(vmem, hbm, hbm),
        scratch_shapes=[
            pltpu.VMEM((16, TILE, 1024), BF16),
            pltpu.VMEM((8, TILE, 1024), BF16),
            pltpu.VMEM((1024, 1024), BF16),
            pltpu.SemaphoreType.DMA((6,)),
            pltpu.SemaphoreType.DMA((6,)),
            pltpu.SemaphoreType.DMA((8,)),
            pltpu.SemaphoreType.DMA((4,)),
        ],
        compiler_params=pltpu.CompilerParams(
            collective_id=0, has_side_effects=True, vmem_limit_bytes=60 << 20
        ),
        name="eliminate",
    )(
        row_tiles, col_tiles, owner.reshape(1, owner.size), pivot,
        border.reshape(16, TILE, 1024), inverse_set,
    )


PARTS = 2
PART = TILE // PARTS


def peer_of(front, z, core, x, u):
    dk, dx, dz, dy = u % 2, (u // 2) % 4, (u // 8) % 4, u // 32
    f2, z2, k2, x2 = (front + dy) % 4, (z + dz) % 4, (core + dk) % 2, (x + dx) % 4
    row, col = (z2 % 2) * 2 + k2, x2 * 2 + z2 // 2
    return f2, row, col


def exchange_kernel(
    tab, own, theirs, contrib, out,
    own_v, theirs_v, theirs_p, contrib_v, left, packed, ordered, lsem, s1, r1, s2, r2, *spread,
):
    front, z_lo, core, x, z_hi = position()
    z = z_hi * 2 + z_lo
    row, col = lax.axis_index("row"), lax.axis_index("col")
    here = row * 8 + col
    everywhere = front * 32 + here
    barrier = pltpu.get_barrier_semaphore()

    def greet(u, _):
        pl.semaphore_signal(barrier, inc=1, device_id=peer_of(front, z, core, x, u), device_id_type=MESH)
        return 0

    lax.fori_loop(1, 128, greet, 0)
    load_theirs = pltpu.make_async_copy(theirs, theirs_v, lsem.at[0])
    load_own = pltpu.make_async_copy(own, own_v, lsem.at[1])
    load_contrib = [
        pltpu.make_async_copy(
            contrib.at[:, :, j * TILE : (j + 1) * TILE], contrib_v.at[j], lsem.at[2 + j]
        )
        for j in range(8)
    ]
    load_theirs.start()
    load_own.start()
    for copy in load_contrib:
        copy.start()
    load_theirs.wait()
    for m in range(8):
        theirs_p[m] = theirs_v[tab[1, m]]
    load_own.wait()
    for copy in load_contrib:
        copy.wait()

    def update(s):
        for q in range(16):
            left[q] = own_v[tab[0, q], s * PART : (s + 1) * PART]

        def two_cols(n, _):
            product = nt(
                left[...].reshape(16 * PART, 1024), theirs_p[pl.ds(n * 2, 2)].reshape(256, 1024)
            )
            for t in range(2):
                for q in range(16):
                    tile = contrib_v[tab[1, 2 * n + t], tab[0, q], s * PART : (s + 1) * PART].astype(F32)
                    part = product[q * PART : (q + 1) * PART, t * TILE : (t + 1) * TILE]
                    packed[s, (q // 4) * 8 + 2 * n + t, q % 4] = (tile - part).astype(BF16)
            return 0

        lax.fori_loop(0, 4, two_cols, 0)

    def first_send(s):
        def send(t, _):
            _, row2, col2 = peer_of(front, z, core, x, (t * 11) % 32)
            pltpu.make_async_remote_copy(
                src_ref=packed.at[s, row2 * 8 + col2], dst_ref=spread[s].at[here],
                send_sem=s1.at[s], recv_sem=r1.at[s],
                device_id=(front, row2, col2), device_id_type=MESH,
            ).start()
            return 0

        lax.fori_loop(1, 32, send, 0)
        spread[s][here] = packed[s, here]

    def first_all(s):
        return pltpu.make_async_remote_copy(
            src_ref=packed.at[s, pl.ds(0, 31)], dst_ref=spread[s].at[pl.ds(0, 31)],
            send_sem=s1.at[s], recv_sem=r1.at[s],
            device_id=(front, row, col), device_id_type=MESH,
        )

    GROUP = 8

    def second_peer(t):
        return peer_of(front, z, core, x, (t * 37) % 128)

    def second_copy(s, t):
        f2, row2, col2 = second_peer(t)
        return pltpu.make_async_remote_copy(
            src_ref=ordered.at[s, t], dst_ref=out.at[s, everywhere],
            send_sem=s2.at[s], recv_sem=r2.at[s],
            device_id=(f2, row2, col2), device_id_type=MESH,
        )

    def second_self(s):
        return pltpu.make_async_copy(ordered.at[s, 0], out.at[s, everywhere], lsem.at[10 + s])

    def second_send(s):
        def fill(t):
            f2, row2, col2 = second_peer(t)
            g = f2 * 4 + row2
            ordered[s, t] = spread[s][tab[2, g] + tab[3, col2], tab[6, g]]

        for t in range(GROUP):
            fill(t)
        second_self(s).start()

        def step(i, _):
            for t in range(GROUP):
                fill(i * GROUP + t)
            for t in range(GROUP):
                at = (i - 1) * GROUP + t

                @pl.when(at > 0)
                def _():
                    second_copy(s, at).start()

            return 0

        lax.fori_loop(1, 128 // GROUP, step, 0)
        for t in range(GROUP):
            second_copy(s, 128 - GROUP + t).start()

    def second_all(s):
        return pltpu.make_async_remote_copy(
            src_ref=ordered.at[s, pl.ds(0, 127)], dst_ref=out.at[s, pl.ds(0, 127)],
            send_sem=s2.at[s], recv_sem=r2.at[s],
            device_id=(front, row, col), device_id_type=MESH,
        )

    for s in range(PARTS):
        update(s)
        if s == 0:
            pl.semaphore_wait(barrier, 127)
        first_send(s)
    for s in range(PARTS):
        first_all(s).wait_recv()
        second_send(s)
    for s in range(PARTS):
        first_all(s).wait_send()
        second_self(s).wait()
        second_all(s).wait_recv()
        second_all(s).wait_send()


def exchanged_update(tables, own, theirs, contrib):
    hbm = pl.BlockSpec(memory_space=pl.ANY)
    return pl.pallas_call(
        exchange_kernel,
        out_shape=jax.ShapeDtypeStruct((PARTS, 128, PART, TILE), BF16),
        in_specs=[pl.BlockSpec(memory_space=pltpu.SMEM), hbm, hbm, hbm],
        out_specs=hbm,
        scratch_shapes=[
            pltpu.VMEM((16, TILE, 1024), BF16),
            pltpu.VMEM((8, TILE, 1024), BF16),
            pltpu.VMEM((8, TILE, 1024), BF16),
            pltpu.VMEM((8, 16, TILE, TILE), BF16),
            pltpu.VMEM((16, PART, 1024), BF16),
            pltpu.VMEM((PARTS, 32, 4, PART, TILE), BF16),
            pltpu.VMEM((PARTS, 128, PART, TILE), BF16),
            pltpu.SemaphoreType.DMA((10 + PARTS,)),
            *[pltpu.SemaphoreType.DMA((PARTS,))] * 4,
            *[pltpu.VMEM((32, 4, PART, TILE), BF16)] * PARTS,
        ],
        compiler_params=pltpu.CompilerParams(
            collective_id=1, has_side_effects=True, vmem_limit_bytes=60 << 20
        ),
        name="exchanged_update",
    )(tables, own, theirs, contrib.reshape(16, TILE, 1024))


def assemble_kernel(tab, t0, t1, t2, t3, init, vectors, schur, partial):
    a = pl.program_id(0)
    tiles = (t0, t1, t2, t3)
    for b in range(10):
        cols = slice(b * TILE, (b + 1) * TILE)
        for s in range(PARTS):
            rows = slice(s * PART, (s + 1) * PART)
            total = init[rows, cols].astype(F32)
            for f in range(4):
                m = tab[5, f * 10 + b]
                there = (m > 0) & (tab[4, f * 5 + a] > 0)
                tile = tiles[f][s, 0, 0, jnp.maximum(m - 1, 0)].astype(F32)
                total = total + jnp.where(there, tile, 0.0)
            schur[rows, cols] = total
    partial[...] = jnp.dot(
        schur[...].astype(BF16), vectors[...], preferred_element_type=F32
    ).astype(partial.dtype)


def assemble(tables, arrived, init, vectors):
    def pick(f):
        return pl.BlockSpec(
            (PARTS, 1, 1, 8, PART, TILE),
            lambda a, tab: (0, f, jnp.maximum(tab[4, f * 5 + a] - 1, 0), 0, 0, 0),
        )

    arrived = arrived.reshape(PARTS, 4, 4, 8, PART, TILE)
    rows, cols = init.shape
    wide = vectors.shape[1]
    return pl.pallas_call(
        assemble_kernel,
        out_shape=(
            jax.ShapeDtypeStruct((rows, cols), F32),
            jax.ShapeDtypeStruct((rows, wide), BF16),
        ),
        grid_spec=pltpu.PrefetchScalarGridSpec(
            num_scalar_prefetch=1,
            grid=(rows // TILE,),
            in_specs=[
                *(pick(f) for f in range(4)),
                pl.BlockSpec((TILE, cols), lambda a, tab: (a, 0)),
                pl.BlockSpec((cols, wide), lambda a, tab: (0, 0)),
            ],
            out_specs=(
                pl.BlockSpec((TILE, cols), lambda a, tab: (a, 0)),
                pl.BlockSpec((TILE, wide), lambda a, tab: (a, 0)),
            ),
        ),
        name="assemble",
    )(tables, arrived, arrived, arrived, arrived, init, vectors)


def product_kernel(partial, out, arrived, ssem, rsem):
    front, row, col = lax.axis_index("front"), lax.axis_index("row"), lax.axis_index("col")
    barrier = pltpu.get_barrier_semaphore()
    others = [(col + d) % 8 for d in range(1, 8)]
    for other in others:
        pl.semaphore_signal(barrier, inc=1, device_id=(front, row, other), device_id_type=MESH)
    pl.semaphore_wait(barrier, 7)
    copies = [
        pltpu.make_async_remote_copy(
            src_ref=partial.at[other], dst_ref=arrived.at[d], send_sem=ssem.at[d], recv_sem=rsem.at[d],
            device_id=(front, row, other), device_id_type=MESH,
        )
        for d, other in enumerate(others)
    ]
    for copy in copies:
        copy.start()
    total = partial[col].astype(F32)
    for d, copy in enumerate(copies):
        copy.wait()
        total = total + arrived[d].astype(F32)
    out[...] = total


def product_sum(partial):
    vmem = pl.BlockSpec(memory_space=pltpu.VMEM)
    _, rows, wide = partial.shape
    return pl.pallas_call(
        product_kernel,
        out_shape=jax.ShapeDtypeStruct((rows, wide), F32),
        in_specs=[vmem],
        out_specs=vmem,
        scratch_shapes=[
            pltpu.VMEM((7, rows, wide), BF16),
            pltpu.SemaphoreType.DMA((7,)),
            pltpu.SemaphoreType.DMA((7,)),
        ],
        compiler_params=pltpu.CompilerParams(collective_id=2, has_side_effects=True),
        name="product_sum",
    )(partial)


def shards(pivot_block, border, contrib, inverses, row_tiles, col_tiles, owner, schur_init, block):
    tables, own, theirs = eliminate(row_tiles, col_tiles, owner, pivot_block, border, inverses)
    arrived = exchanged_update(tables, own, theirs, contrib)
    schur, partial = assemble(tables, arrived, schur_init, block)
    return schur, product_sum(partial.reshape(8, 80, 512))


def solution(mesh):
    in_specs = (
        P("front", None, None),
        P("front", "row", None),
        P("front", "row", "col"),
        P("front", None, None, None),
        P(),
        P(),
        P(),
        P(("front", "row"), "col"),
        P("col", None),
    )
    out_specs = (P(("front", "row"), "col"), P(("front", "row", "col"), None))
    return jax.shard_map(shards, mesh=mesh, in_specs=in_specs, out_specs=out_specs, check_vma=False)
```

```python
import functools

import jax
import jax.numpy as jnp
from jax import lax
from jax.experimental import pallas as pl
from jax.experimental.pallas import tpu as pltpu
from jax.sharding import PartitionSpec as P

TILE = 128
MESH = pl.DeviceIdType.MESH
F32 = jnp.float32
BF16 = jnp.bfloat16


def nt(a, b):
    return lax.dot_general(a, b, (((1,), (1,)), ((), ())), preferred_element_type=F32)


def split_levels(src_c, src_r, dst_c, dst_r, squarings):
    n = src_c.shape[0]
    at_c = lax.broadcasted_iota(jnp.int32, (n, n), 0).astype(F32)
    at_r = lax.broadcasted_iota(jnp.int32, (n, n), 1).astype(F32)
    color_c = jnp.zeros((n, 1), F32)
    color_r = jnp.zeros((1, n), F32)

    def partners(node_c, node_r):
        same = jnp.where((node_c == node_r) & (color_c == color_r), 1.0, 0.0)
        rank_c = jnp.sum(jnp.where(at_r < at_c, same, 0.0), axis=1, keepdims=True)
        rank_r = jnp.sum(jnp.where(at_c < at_r, same, 0.0), axis=0, keepdims=True)
        pair = (jnp.floor(rank_c * 0.5) == jnp.floor(rank_r * 0.5)) & (at_c != at_r)
        return jnp.where(pair, same, 0.0)

    for count in squarings:
        by_src = partners(src_c, src_r)
        by_dst = partners(dst_c, dst_r)
        reach = jnp.dot(by_src.astype(BF16), by_dst.astype(BF16), preferred_element_type=F32)
        reach = jnp.where(at_c == at_r, 1.0, reach)
        for _ in range(count):
            half = reach.astype(BF16)
            reach = jnp.where(jnp.dot(half, half, preferred_element_type=F32) > 0.5, 1.0, 0.0)
        far = float(n)
        label_c = jnp.min(jnp.where(reach > 0.5, at_r, far), axis=1, keepdims=True)
        label_r = jnp.min(jnp.where(reach > 0.5, at_c, far), axis=0, keepdims=True)
        other_c = jnp.sum(by_src * label_r, axis=1, keepdims=True)
        other_r = jnp.sum(by_src * label_c, axis=0, keepdims=True)
        color_c = color_c * 2.0 + jnp.where(label_c > other_c, 1.0, 0.0)
        color_r = color_r * 2.0 + jnp.where(label_r > other_r, 1.0, 0.0)
    return color_c


def div(x, by):
    return jnp.floor((x + 0.5) * (1.0 / by))


def routing(rows_c, rows_r, cols_c, cols_r, owner_r, owner_c, front, row, col):
    n = rows_c.shape[0]
    per = n // 4
    slots = owner_r.shape[1]
    lane = lax.broadcasted_iota(jnp.int32, (n, slots), 1)
    sub = lax.broadcasted_iota(jnp.int32, (slots, n), 0)
    own_r = owner_r.astype(F32)
    own_c = owner_c.astype(F32)

    def slot_c(ids):
        return jnp.sum(jnp.where(ids == lane, own_r, 0.0), axis=1, keepdims=True)

    def slot_r(ids):
        return jnp.sum(jnp.where(ids == sub, own_c, 0.0), axis=0, keepdims=True)

    e_c = lax.broadcasted_iota(jnp.int32, (n, 1), 0).astype(F32)
    e_r = lax.broadcasted_iota(jnp.int32, (1, n), 1).astype(F32)
    f_c, f_r = div(e_c, per), div(e_r, per)
    i_c = e_c - f_c * per
    rs_c, rs_r, cs_c, cs_r = slot_c(rows_c), slot_r(rows_r), slot_c(cols_c), slot_r(cols_r)
    g_c, g_r, h_c, h_r = div(rs_c, 5), div(rs_r, 5), div(cs_c, 10), div(cs_r, 10)
    a_c, b_c = rs_c - g_c * 5, cs_c - h_c * 10
    mr = split_levels(div(e_c, 4), div(e_r, 4), f_c * 16 + g_c, f_r * 16 + g_r, (5, 4))
    mc = split_levels(div(e_c, 8), div(e_r, 8), f_c * 8 + h_c, f_r * 8 + h_r, (5, 4, 3))
    front, row, col = front.astype(F32), row.astype(F32), col.astype(F32)
    mine = f_c == front
    q = lax.broadcasted_iota(jnp.int32, (n, TILE), 1).astype(F32)

    def table(mask, value):
        return jnp.sum(jnp.where(mask, value, 0.0), axis=0, keepdims=True)

    in_row = i_c - div(i_c, 16) * 16
    chunk = div(in_row, 4)
    t0 = table(mine & (div(i_c, 16) == row) & (mr * 4 + chunk == q), in_row)
    block = div(i_c, 8)
    t1 = table(mine & (block == col) & (mc == q), i_c - block * 8)
    at_row = mine & (mr == row) & (g_c == q)
    t2 = table(at_row, div(i_c, 16) * 8)
    t3 = table(mine & (mc == col) & (h_c == q), block)
    t6 = table(at_row, chunk)
    t4 = table((g_c == front * 4 + row) & (f_c * 5 + a_c == q), mr + 1.0)
    t5 = table((h_c == col) & (f_c * 10 + b_c == q), mc + 1.0)
    zero = jnp.zeros_like(t0)
    return jnp.concatenate([t0, t1, t2, t3, t4, t5, t6, zero], axis=0).astype(jnp.int32)


def both_ways(ids):
    fronts, per = ids.shape
    n = fronts * per
    spread = jnp.where(
        lax.broadcasted_iota(jnp.int32, (per, n), 0) == lax.broadcasted_iota(jnp.int32, (per, n), 1) % per, 1.0, 0.0
    )
    wide = jnp.dot(ids.astype(F32).astype(BF16), spread.astype(BF16), preferred_element_type=F32)
    here = lax.broadcasted_iota(jnp.int32, (fronts, n), 0) == lax.broadcasted_iota(jnp.int32, (fronts, n), 1) // per
    flat = jnp.sum(jnp.where(here, wide, 0.0), axis=0, keepdims=True)
    return turned(flat).astype(jnp.int32), flat.astype(jnp.int32)


def turned(flat):
    n = flat.shape[1]
    eye = lax.broadcasted_iota(jnp.int32, (n, n), 0) == lax.broadcasted_iota(jnp.int32, (n, n), 1)
    return jnp.sum(jnp.where(eye, flat, 0.0), axis=1, keepdims=True)


def position():
    front, row, col = lax.axis_index("front"), lax.axis_index("row"), lax.axis_index("col")
    return front, row // 2, row % 2, col // 2, col % 2


def device(front, z, core, x):
    return (front, (z % 2) * 2 + core, x * 2 + z // 2)


def eliminate_rows(block, lower, inverse_set):
    parts = []
    for k in range(4):
        now = block[:, k * 256 : (k + 1) * 256].astype(F32)
        for j in range(k):
            now = now - nt(parts[j], lower[k * 256 : (k + 1) * 256, j * 256 : (j + 1) * 256])
        parts.append(
            jnp.dot(now.astype(BF16), inverse_set[k], preferred_element_type=F32).astype(BF16)
        )
    return parts


def eliminate_kernel(
    row_tiles, col_tiles, owner, pivot, border, inverse_set, tab, own_out, theirs_out,
    rows_v, theirs, lower, lsem, osem, ssem, rsem,
):
    front, z_lo, core, x, z_hi = position()
    z = z_hi * 2 + z_lo
    up, down = (z + 1) % 4, (z + 3) % 4
    on_source_chip = z_lo == x // 2
    is_source = on_source_chip & (core == x % 2)
    sibling = device(front, z, 1 - core, x)
    barrier = pltpu.get_barrier_semaphore()
    for peer in (sibling, *(device(front, zz, k, x) for zz in (up, down) for k in (0, 1))):
        pl.semaphore_signal(barrier, inc=1, device_id=peer, device_id_type=MESH)
    load_lower = pltpu.make_async_copy(pivot.at[0], lower, lsem.at[0])
    load_rows = pltpu.make_async_copy(border, rows_v, lsem.at[1])
    load_lower.start()
    load_rows.start()
    pl.semaphore_wait(barrier, 5)

    def push(src, quarter, sem, peer):
        return pltpu.make_async_remote_copy(
            src_ref=src, dst_ref=theirs.at[pl.ds(2 * quarter, 2)], send_sem=ssem.at[sem],
            recv_sem=rsem.at[quarter], device_id=peer, device_id_type=MESH,
        )

    def quarter_of(half, q):
        return border.at[pl.ds(half * 8 + q * 2, 2)]

    def source_sends():
        sends = []
        for q in (0, 1):
            sends.append(push(quarter_of(up // 2, q), q, q, device(front, up, q, x)))
            sends.append(push(quarter_of(down // 2, 2 + q), 2 + q, 2 + q, device(front, down, q, x)))
        for q in range(4):
            sends.append(push(quarter_of(z_hi, q), q, 4 + q, sibling))
        return sends

    def own_quarters():
        return [
            pltpu.make_async_copy(quarter_of(z_hi, q), theirs.at[pl.ds(2 * q, 2)], lsem.at[2 + q])
            for q in range(4)
        ]

    @pl.when(is_source)
    def _():
        for copy in source_sends():
            copy.start()
        for copy in own_quarters():
            copy.start()

    load_lower.wait()
    for k in range(3):
        low = (k + 1) * 256
        now = lower[low:, k * 256 : (k + 1) * 256].astype(F32)
        for j in range(k):
            now = now - nt(
                lower[low:, j * 256 : (j + 1) * 256], lower[k * 256 : low, j * 256 : (j + 1) * 256]
            )
        lower[low:, k * 256 : (k + 1) * 256] = jnp.dot(
            now.astype(BF16), inverse_set[0, k], preferred_element_type=F32
        ).astype(BF16)
    load_rows.wait()

    def block_of(buffer, target, base):
        def step(i, _):
            rows = pl.ds(i * 4, 4)
            parts = eliminate_rows(buffer[rows].reshape(512, 1024), lower, inverse_set.at[0])
            for k in range(4):
                buffer[rows, :, k * 256 : (k + 1) * 256] = parts[k].reshape(4, TILE, 256)
            pltpu.make_async_copy(buffer.at[rows], target.at[rows], osem.at[base + i]).start()
            return 0

        return step

    lax.fori_loop(0, 4, block_of(rows_v, own_out, 0), 0)
    rows_c, rows_r = both_ways(row_tiles[...])
    cols_c, cols_r = both_ways(col_tiles[...])
    tab[...] = routing(
        rows_c, rows_r, cols_c, cols_r, owner[...], turned(owner[...].astype(F32)),
        front, lax.axis_index("row"), lax.axis_index("col"),
    )

    def wait_quarter(q):
        push(theirs.at[pl.ds(2 * q, 2)], q, 0, sibling).wait_recv()

    def forwards():
        return [
            push(theirs.at[pl.ds(2 * q, 2)], q, i, sibling) for i, q in enumerate((core, 2 + core))
        ]

    @pl.when(is_source)
    def _():
        for copy in own_quarters():
            copy.wait()

    @pl.when(jnp.logical_not(on_source_chip))
    def _():
        first, second = forwards()
        wait_quarter(core)
        first.start()
        wait_quarter(2 + core)
        second.start()
        wait_quarter(1 - core)
        wait_quarter(3 - core)

    @pl.when(on_source_chip & jnp.logical_not(is_source))
    def _():
        for q in range(4):
            wait_quarter(q)

    @pl.when(is_source)
    def _():
        for copy in source_sends():
            copy.wait_send()

    @pl.when(jnp.logical_not(on_source_chip))
    def _():
        for copy in forwards():
            copy.wait_send()

    lax.fori_loop(0, 2, block_of(theirs, theirs_out, 4), 0)
    for i in range(4):
        rows = pl.ds(i * 4, 4)
        pltpu.make_async_copy(rows_v.at[rows], own_out.at[rows], osem.at[i]).wait()
    for i in range(2):
        rows = pl.ds(i * 4, 4)
        pltpu.make_async_copy(theirs.at[rows], theirs_out.at[rows], osem.at[4 + i]).wait()


def eliminate(row_tiles, col_tiles, owner, pivot, border, inverse_set):
    vmem = pl.BlockSpec(memory_space=pltpu.VMEM)
    hbm = pl.BlockSpec(memory_space=pl.ANY)
    return pl.pallas_call(
        eliminate_kernel,
        out_shape=(
            jax.ShapeDtypeStruct((8, TILE), jnp.int32),
            jax.ShapeDtypeStruct((16, TILE, 1024), BF16),
            jax.ShapeDtypeStruct((8, TILE, 1024), BF16),
        ),
        in_specs=[vmem, vmem, vmem, hbm, hbm, vmem],
        out_specs=(vmem, hbm, hbm),
        scratch_shapes=[
            pltpu.VMEM((16, TILE, 1024), BF16),
            pltpu.VMEM((8, TILE, 1024), BF16),
            pltpu.VMEM((1024, 1024), BF16),
            pltpu.SemaphoreType.DMA((6,)),
            pltpu.SemaphoreType.DMA((6,)),
            pltpu.SemaphoreType.DMA((8,)),
            pltpu.SemaphoreType.DMA((4,)),
        ],
        compiler_params=pltpu.CompilerParams(
            collective_id=0, has_side_effects=True, vmem_limit_bytes=60 << 20
        ),
        name="eliminate",
    )(
        row_tiles, col_tiles, owner.reshape(1, owner.size), pivot,
        border.reshape(16, TILE, 1024), inverse_set,
    )


PARTS = 8


ORDER1 = 11
ORDER2 = 37


def peer_of(front, z, core, x, u):
    dk, dx, dz, dy = u & 1, (u >> 1) & 3, (u >> 3) & 3, u >> 5
    f2, z2, k2, x2 = (front + dy) & 3, (z + dz) & 3, core ^ dk, (x + dx) & 3
    return f2, ((z2 & 1) << 1) + k2, (x2 << 1) + (z2 >> 1)


GROUP = 8
UNIT = 16


def exchange_kernel(
    tab, own, theirs, contrib, init, vectors, schur, product,
    own_v, theirs_v, theirs_p, contrib_v, left, packed, ordered, init_v, vectors_v, schur_v, rounded, partial, sums,
    lsem, s1, r1, s2, r2, osem, s3, r3, *buffers,
):
    spread, landed = buffers[:PARTS], buffers[PARTS:]
    size = TILE // PARTS
    units = size // UNIT
    front, z_lo, core, x, z_hi = position()
    z = z_hi * 2 + z_lo
    row, col = lax.axis_index("row"), lax.axis_index("col")
    here = row * 8 + col
    everywhere = front * 32 + here
    barrier = pltpu.get_barrier_semaphore()

    def greet(u, _):
        pl.semaphore_signal(barrier, inc=1, device_id=peer_of(front, z, core, x, u), device_id_type=MESH)
        return 0

    lax.fori_loop(1, 128, greet, 0)
    load_theirs = pltpu.make_async_copy(theirs, theirs_v, lsem.at[0])
    load_own = pltpu.make_async_copy(own, own_v, lsem.at[1])
    load_contrib = [
        pltpu.make_async_copy(
            contrib.at[:, :, j * TILE : (j + 1) * TILE], contrib_v.at[j], lsem.at[4 + j]
        )
        for j in range(8)
    ]
    load_init = pltpu.make_async_copy(init, init_v, lsem.at[2])
    load_vectors = pltpu.make_async_copy(vectors, vectors_v, lsem.at[3])
    load_theirs.start()
    load_own.start()
    for copy in load_contrib:
        copy.start()
    load_init.start()
    load_vectors.start()
    load_theirs.wait()
    for m in range(8):
        theirs_p[m] = theirs_v[tab[1, m]]
    load_own.wait()
    for copy in load_contrib:
        copy.wait()

    def update(s):
        rows = slice(s * size, (s + 1) * size)
        for q in range(16):
            left[q] = own_v[tab[0, q], rows]

        def two_cols(n, _):
            product = nt(
                left[...].reshape(16 * size, 1024), theirs_p[pl.ds(n * 2, 2)].reshape(256, 1024)
            )
            for t in range(2):
                for q in range(16):
                    tile = contrib_v[tab[1, 2 * n + t], tab[0, q], rows].astype(F32)
                    part = product[q * size : (q + 1) * size, t * TILE : (t + 1) * TILE]
                    packed[s, (q // 4) * 8 + 2 * n + t, q % 4] = (tile - part).astype(BF16)
            return 0

        lax.fori_loop(0, 4, two_cols, 0)

    def first_send(s):
        def send(t, _):
            _, row2, col2 = peer_of(front, z, core, x, (t * ORDER1) & 31)
            pltpu.make_async_remote_copy(
                src_ref=packed.at[s, row2 * 8 + col2], dst_ref=spread[s].at[here],
                send_sem=s1.at[s], recv_sem=r1.at[s],
                device_id=(front, row2, col2), device_id_type=MESH,
            ).start()
            return 0

        lax.fori_loop(1, 32, send, 0)
        spread[s][here] = packed[s, here]

    def first_all(s):
        return pltpu.make_async_remote_copy(
            src_ref=packed.at[s, pl.ds(0, 31)], dst_ref=spread[s].at[pl.ds(0, 31)],
            send_sem=s1.at[s], recv_sem=r1.at[s],
            device_id=(front, row, col), device_id_type=MESH,
        )

    def second_peer(t):
        return peer_of(front, z, core, x, (t * ORDER2) & 127)

    def second_copy(s, t):
        return pltpu.make_async_remote_copy(
            src_ref=ordered.at[s, t], dst_ref=landed[s].at[everywhere],
            send_sem=s2.at[s], recv_sem=r2.at[s],
            device_id=second_peer(t), device_id_type=MESH,
        )

    def second_send(s):
        def fill(t):
            f2, row2, col2 = second_peer(t)
            g = f2 * 4 + row2
            ordered[s, t] = spread[s][tab[2, g] + tab[3, col2], tab[6, g]]

        for t in range(GROUP):
            fill(t)
        landed[s][everywhere] = ordered[s, 0]
        for t in range(1, GROUP):
            second_copy(s, t).start()

        def step(i, _):
            for t in range(GROUP):
                fill(i * GROUP + t)
            for t in range(GROUP):
                second_copy(s, i * GROUP + t).start()
            return 0

        lax.fori_loop(1, 128 // GROUP, step, 0)

    def second_all(s):
        return pltpu.make_async_remote_copy(
            src_ref=ordered.at[s, pl.ds(0, 127)], dst_ref=landed[s].at[pl.ds(0, 127)],
            send_sem=s2.at[s], recv_sem=r2.at[s],
            device_id=(front, row, col), device_id_type=MESH,
        )

    def strip(a, s):
        return pl.ds(a * TILE + s * size, size)

    def write(a, s):
        return pltpu.make_async_copy(schur_v.at[strip(a, s)], schur.at[strip(a, s)], osem.at[s, a])

    def assemble(s):
        def row_of_tiles(a, _):
            rows = pl.ds(pl.multiple_of(a * TILE + s * size, size), size)
            for b in range(10):
                cols = slice(b * TILE, (b + 1) * TILE)
                total = init_v[rows, cols].astype(F32)
                for f in range(4):
                    m, k = tab[4, f * 5 + a], tab[5, f * 10 + b]
                    at = f * 32 + jnp.maximum(m - 1, 0) * 8 + jnp.maximum(k - 1, 0)
                    total = total + jnp.where((m > 0) & (k > 0), landed[s][at].astype(F32), 0.0)
                schur_v[rows, cols] = total
                rounded[pl.ds(pl.multiple_of(a * size, size), size), cols] = total.astype(BF16)
            return 0

        lax.fori_loop(0, 5, row_of_tiles, 0)
        for a in range(5):
            write(a, s).start()
        partial[s] = (
            jnp.dot(rounded[...], vectors_v[...], preferred_element_type=F32)
            .astype(BF16)
            .reshape(5, units, UNIT, partial.shape[-1])
        )

    def product_copies(s):
        copies = []
        for a in range(5):
            for j in range(units):
                u = (a * TILE + s * size) // UNIT + j
                copies.append(
                    (
                        u // 5,
                        u % 5,
                        partial.at[s, a, j],
                        pltpu.make_async_remote_copy(
                            src_ref=partial.at[s, a, j], dst_ref=sums.at[col, u % 5],
                            send_sem=s3, recv_sem=r3,
                            device_id=(front, row, u // 5), device_id_type=MESH,
                        ),
                    )
                )
        return copies

    def product_send(s):
        for to, at, value, copy in product_copies(s):

            @pl.when(col != to)
            def _():
                copy.start()

            @pl.when(col == to)
            def _():
                sums[to, at] = value[...]

    def product_all():
        return pltpu.make_async_remote_copy(
            src_ref=sums.at[pl.ds(0, 7)], dst_ref=sums.at[pl.ds(0, 7)], send_sem=s3, recv_sem=r3,
            device_id=(front, row, col), device_id_type=MESH,
        )

    for s in range(PARTS):
        update(s)
        if s == 0:
            pl.semaphore_wait(barrier, 127)
        first_send(s)
    for s in range(PARTS):
        first_all(s).wait_recv()
        second_send(s)
    load_init.wait()
    load_vectors.wait()
    for s in range(PARTS):
        second_all(s).wait_recv()
        assemble(s)
        product_send(s)
    for s in range(PARTS):
        first_all(s).wait_send()
        second_all(s).wait_send()
    product_all().wait_recv()
    total = sums[0].astype(F32)
    for c in range(1, 8):
        total = total + sums[c].astype(F32)
    product[...] = total.reshape(product.shape)
    product_all().wait_send()
    for s in range(PARTS):
        for a in range(5):
            write(a, s).wait()


def exchanged_update(tables, own, theirs, contrib, init, vectors):
    hbm = pl.BlockSpec(memory_space=pl.ANY)
    size = TILE // PARTS
    rows, cols = init.shape
    wide = vectors.shape[1]
    return pl.pallas_call(
        exchange_kernel,
        out_shape=(
            jax.ShapeDtypeStruct((rows, cols), F32),
            jax.ShapeDtypeStruct((rows // 8, wide), F32),
        ),
        in_specs=[pl.BlockSpec(memory_space=pltpu.SMEM), hbm, hbm, hbm, hbm, hbm],
        out_specs=(hbm, pl.BlockSpec(memory_space=pltpu.VMEM)),
        scratch_shapes=[
            pltpu.VMEM((16, TILE, 1024), BF16),
            pltpu.VMEM((8, TILE, 1024), BF16),
            pltpu.VMEM((8, TILE, 1024), BF16),
            pltpu.VMEM((8, 16, TILE, TILE), BF16),
            pltpu.VMEM((16, size, 1024), BF16),
            pltpu.VMEM((PARTS, 32, 4, size, TILE), BF16),
            pltpu.VMEM((PARTS, 128, size, TILE), BF16),
            pltpu.VMEM((rows, cols), BF16),
            pltpu.VMEM((cols, wide), BF16),
            pltpu.VMEM((rows, cols), F32),
            pltpu.VMEM((5 * size, cols), BF16),
            pltpu.VMEM((PARTS, 5, size // UNIT, UNIT, wide), BF16),
            pltpu.VMEM((8, 5, UNIT, wide), BF16),
            pltpu.SemaphoreType.DMA((12,)),
            *[pltpu.SemaphoreType.DMA((PARTS,))] * 4,
            pltpu.SemaphoreType.DMA((PARTS, 5)),
            pltpu.SemaphoreType.DMA,
            pltpu.SemaphoreType.DMA,
            *[pltpu.VMEM((32, 4, size, TILE), BF16)] * PARTS,
            *[pltpu.VMEM((128, size, TILE), BF16)] * PARTS,
        ],
        compiler_params=pltpu.CompilerParams(
            collective_id=1, has_side_effects=True, vmem_limit_bytes=60 << 20
        ),
        name="exchanged_update",
    )(tables, own, theirs, contrib.reshape(16, TILE, 1024), init, vectors)


def shards(pivot_block, border, contrib, inverses, row_tiles, col_tiles, owner, schur_init, block):
    tables, own, theirs = eliminate(row_tiles, col_tiles, owner, pivot_block, border, inverses)
    return exchanged_update(tables, own, theirs, contrib, schur_init, block)


def solution(mesh):
    in_specs = (
        P("front", None, None),
        P("front", "row", None),
        P("front", "row", "col"),
        P("front", None, None, None),
        P(),
        P(),
        P(),
        P(("front", "row"), "col"),
        P("col", None),
    )
    out_specs = (P(("front", "row"), "col"), P(("front", "row", "col"), None))
    return jax.shard_map(shards, mesh=mesh, in_specs=in_specs, out_specs=out_specs, check_vma=False)
```

```python
import functools

import jax
import jax.numpy as jnp
from jax import lax
from jax.experimental import pallas as pl
from jax.experimental.pallas import tpu as pltpu
from jax.sharding import PartitionSpec as P

TILE = 128
MESH = pl.DeviceIdType.MESH
F32 = jnp.float32
BF16 = jnp.bfloat16


def within(index, last):
    return jnp.minimum(jnp.maximum(index, 0), last)


def nt(a, b):
    return lax.dot_general(a, b, (((1,), (1,)), ((), ())), preferred_element_type=F32)


def split_levels(src_c, src_r, dst_c, dst_r, squarings):
    n = src_c.shape[0]
    at_c = lax.broadcasted_iota(jnp.int32, (n, n), 0).astype(F32)
    at_r = lax.broadcasted_iota(jnp.int32, (n, n), 1).astype(F32)
    color_c = jnp.zeros((n, 1), F32)
    color_r = jnp.zeros((1, n), F32)

    def partners(node_c, node_r):
        same = jnp.where((node_c == node_r) & (color_c == color_r), 1.0, 0.0)
        rank_c = jnp.sum(jnp.where(at_r < at_c, same, 0.0), axis=1, keepdims=True)
        rank_r = jnp.sum(jnp.where(at_c < at_r, same, 0.0), axis=0, keepdims=True)
        pair = (jnp.floor(rank_c * 0.5) == jnp.floor(rank_r * 0.5)) & (at_c != at_r)
        return jnp.where(pair, same, 0.0)

    for count in squarings:
        by_src = partners(src_c, src_r)
        by_dst = partners(dst_c, dst_r)
        reach = jnp.dot(by_src.astype(BF16), by_dst.astype(BF16), preferred_element_type=F32)
        reach = jnp.where(at_c == at_r, 1.0, reach)
        for _ in range(count):
            half = reach.astype(BF16)
            reach = jnp.where(jnp.dot(half, half, preferred_element_type=F32) > 0.5, 1.0, 0.0)
        far = float(n)
        label_c = jnp.min(jnp.where(reach > 0.5, at_r, far), axis=1, keepdims=True)
        label_r = jnp.min(jnp.where(reach > 0.5, at_c, far), axis=0, keepdims=True)
        other_c = jnp.sum(by_src * label_r, axis=1, keepdims=True)
        other_r = jnp.sum(by_src * label_c, axis=0, keepdims=True)
        color_c = color_c * 2.0 + jnp.where(label_c > other_c, 1.0, 0.0)
        color_r = color_r * 2.0 + jnp.where(label_r > other_r, 1.0, 0.0)
    return color_c


def div(x, by):
    return jnp.floor((x + 0.5) * (1.0 / by))


def routing(rows_c, rows_r, cols_c, cols_r, owner_r, owner_c, front, row, col):
    n = rows_c.shape[0]
    per = n // 4
    slots = owner_r.shape[1]
    lane = lax.broadcasted_iota(jnp.int32, (n, slots), 1)
    sub = lax.broadcasted_iota(jnp.int32, (slots, n), 0)
    own_r = owner_r.astype(F32)
    own_c = owner_c.astype(F32)

    def slot_c(ids):
        return jnp.sum(jnp.where(ids == lane, own_r, 0.0), axis=1, keepdims=True)

    def slot_r(ids):
        return jnp.sum(jnp.where(ids == sub, own_c, 0.0), axis=0, keepdims=True)

    e_c = lax.broadcasted_iota(jnp.int32, (n, 1), 0).astype(F32)
    e_r = lax.broadcasted_iota(jnp.int32, (1, n), 1).astype(F32)
    f_c, f_r = div(e_c, per), div(e_r, per)
    i_c = e_c - f_c * per
    rs_c, rs_r, cs_c, cs_r = slot_c(rows_c), slot_r(rows_r), slot_c(cols_c), slot_r(cols_r)
    g_c, g_r, h_c, h_r = div(rs_c, 5), div(rs_r, 5), div(cs_c, 10), div(cs_r, 10)
    a_c, b_c = rs_c - g_c * 5, cs_c - h_c * 10
    mr = split_levels(div(e_c, 4), div(e_r, 4), f_c * 16 + g_c, f_r * 16 + g_r, (5, 4))
    mc = split_levels(div(e_c, 8), div(e_r, 8), f_c * 8 + h_c, f_r * 8 + h_r, (5, 4, 3))
    front, row, col = front.astype(F32), row.astype(F32), col.astype(F32)
    mine = f_c == front
    q = lax.broadcasted_iota(jnp.int32, (n, TILE), 1).astype(F32)

    def table(mask, value):
        return jnp.sum(jnp.where(mask, value, 0.0), axis=0, keepdims=True)

    in_row = i_c - div(i_c, 16) * 16
    chunk = div(in_row, 4)
    t0 = table(mine & (div(i_c, 16) == row) & (mr * 4 + chunk == q), in_row)
    block = div(i_c, 8)
    t1 = table(mine & (block == col) & (mc == q), i_c - block * 8)
    at_row = mine & (mr == row) & (g_c == q)
    t2 = table(at_row, div(i_c, 16) * 8)
    t3 = table(mine & (mc == col) & (h_c == q), block)
    t6 = table(at_row, chunk)
    t4 = table((g_c == front * 4 + row) & (f_c * 5 + a_c == q), mr + 1.0)
    t5 = table((h_c == col) & (f_c * 10 + b_c == q), mc + 1.0)
    zero = jnp.zeros_like(t0)
    tops = (15.0, 7.0, 24.0, 7.0, 4.0, 8.0, 3.0, 0.0)
    tables = [jnp.minimum(t, top) for t, top in zip((t0, t1, t2, t3, t4, t5, t6, zero), tops)]
    return jnp.concatenate(tables, axis=0).astype(jnp.int32)


def both_ways(ids):
    fronts, per = ids.shape
    n = fronts * per
    spread = jnp.where(
        lax.broadcasted_iota(jnp.int32, (per, n), 0) == lax.broadcasted_iota(jnp.int32, (per, n), 1) % per, 1.0, 0.0
    )
    wide = jnp.dot(ids.astype(F32).astype(BF16), spread.astype(BF16), preferred_element_type=F32)
    here = lax.broadcasted_iota(jnp.int32, (fronts, n), 0) == lax.broadcasted_iota(jnp.int32, (fronts, n), 1) // per
    flat = jnp.sum(jnp.where(here, wide, 0.0), axis=0, keepdims=True)
    return turned(flat).astype(jnp.int32), flat.astype(jnp.int32)


def turned(flat):
    n = flat.shape[1]
    eye = lax.broadcasted_iota(jnp.int32, (n, n), 0) == lax.broadcasted_iota(jnp.int32, (n, n), 1)
    return jnp.sum(jnp.where(eye, flat, 0.0), axis=1, keepdims=True)


def position():
    front, row, col = lax.axis_index("front"), lax.axis_index("row"), lax.axis_index("col")
    return front, row // 2, row % 2, col // 2, col % 2


def device(front, z, core, x):
    return (front, (z % 2) * 2 + core, x * 2 + z // 2)


def eliminate_rows(block, lower, inverse_set):
    parts = []
    for k in range(4):
        now = block[:, k * 256 : (k + 1) * 256].astype(F32)
        for j in range(k):
            now = now - nt(parts[j], lower[k * 256 : (k + 1) * 256, j * 256 : (j + 1) * 256])
        parts.append(
            jnp.dot(now.astype(BF16), inverse_set[k], preferred_element_type=F32).astype(BF16)
        )
    return parts


PARTS = 8


ORDER1 = 11
ORDER2 = 37


def peer_of(front, z, core, x, u):
    dk, dx, dz, dy = u & 1, (u >> 1) & 3, (u >> 3) & 3, u >> 5
    f2, z2, k2, x2 = (front + dy) & 3, (z + dz) & 3, core ^ dk, (x + dx) & 3
    return f2, ((z2 & 1) << 1) + k2, (x2 << 1) + (z2 >> 1)


GROUP = 8
UNIT = 16


def front_kernel(
    row_tiles, col_tiles, owner, pivot, border, contrib, inverse_set, init, vectors, schur, product,
    tab_v, tab, rows_v, theirs, theirs_e, theirs_p, lower, contrib_v, left, packed, ordered, init_v, vectors_v, schur_v,
    rounded, partial, sums, bsend, brecv, lsem, s1, r1, s2, r2, osem, s3, r3, *buffers,
):
    spread, landed = buffers[:PARTS], buffers[PARTS:]
    size = TILE // PARTS
    units = size // UNIT
    front, z_lo, core, x, z_hi = position()
    z = z_hi * 2 + z_lo
    row, col = lax.axis_index("row"), lax.axis_index("col")
    here = row * 8 + col
    everywhere = front * 32 + here
    up, down = (z + 1) & 3, (z + 3) & 3
    on_source_chip = z_lo == x // 2
    is_source = on_source_chip & (core == x % 2)
    sibling = device(front, z, 1 - core, x)
    barrier = pltpu.get_barrier_semaphore()

    def greet(u, _):
        pl.semaphore_signal(barrier, inc=1, device_id=peer_of(front, z, core, x, u), device_id_type=MESH)
        return 0

    lax.fori_loop(1, 128, greet, 0)
    load_lower = pltpu.make_async_copy(pivot.at[0], lower, lsem.at[0])
    load_rows = pltpu.make_async_copy(border, rows_v, lsem.at[1])
    load_init = pltpu.make_async_copy(init, init_v, lsem.at[2])
    load_vectors = pltpu.make_async_copy(vectors, vectors_v, lsem.at[3])
    load_contrib = [
        pltpu.make_async_copy(
            contrib.at[:, :, j * TILE : (j + 1) * TILE], contrib_v.at[j], lsem.at[4 + j]
        )
        for j in range(8)
    ]
    load_lower.start()
    load_rows.start()
    pl.semaphore_wait(barrier, 127)

    def push(src, tile, sem, peer):
        return pltpu.make_async_remote_copy(
            src_ref=src, dst_ref=theirs.at[tile], send_sem=bsend.at[sem], recv_sem=brecv.at[tile],
            device_id=peer, device_id_type=MESH,
        )

    def source_sends():
        sends = []
        for tile in (0, 2, 1, 3, 4, 6, 5, 7):
            to = down if tile & 2 else up
            sends.append(push(border.at[(to >> 1) * 8 + tile], tile, tile, device(front, to, tile & 1, x)))
        for tile in range(8):
            sends.append(push(border.at[z_hi * 8 + tile], tile, 8 + tile, sibling))
        return sends

    def own_tiles(first, last):
        return [
            pltpu.make_async_copy(border.at[z_hi * 8 + t], theirs.at[t], lsem.at[12 + t]) for t in range(first, last)
        ]

    @pl.when(is_source)
    def _():
        for copy in source_sends():
            copy.start()
        for copy in own_tiles(0, 8):
            copy.start()

    for copy in load_contrib:
        copy.start()
    load_init.start()
    load_vectors.start()
    rows_c, rows_r = both_ways(row_tiles[...])
    cols_c, cols_r = both_ways(col_tiles[...])
    tab_v[...] = routing(
        rows_c, rows_r, cols_c, cols_r, owner[...], turned(owner[...].astype(F32)), front, row, col
    )
    load_lower.wait()
    for k in range(3):
        low = (k + 1) * 256
        now = lower[low:, k * 256 : (k + 1) * 256].astype(F32)
        for j in range(k):
            now = now - nt(
                lower[low:, j * 256 : (j + 1) * 256], lower[k * 256 : low, j * 256 : (j + 1) * 256]
            )
        lower[low:, k * 256 : (k + 1) * 256] = jnp.dot(
            now.astype(BF16), inverse_set[0, k], preferred_element_type=F32
        ).astype(BF16)
    load_rows.wait()

    def block_of(source, target):
        def step(i, _):
            rows = pl.ds(i * 4, 4)
            parts = eliminate_rows(source[rows].reshape(512, 1024), lower, inverse_set.at[0])
            for k in range(4):
                target[rows, :, k * 256 : (k + 1) * 256] = parts[k].reshape(4, TILE, 256)
            return 0

        return step

    lax.fori_loop(0, 4, block_of(rows_v, rows_v), 0)
    table_copy = pltpu.make_async_copy(tab_v, tab, lsem.at[20])
    table_copy.start()

    def wait_tile(t):
        push(theirs.at[t], t, 0, sibling).wait_recv()

    def forward(t):
        return push(theirs.at[t], t, t >> 1, sibling)

    for i in range(2):
        base = 4 * i

        @pl.when(is_source)
        def _():
            for copy in own_tiles(base, base + 4):
                copy.wait()

        @pl.when(jnp.logical_not(on_source_chip))
        def _():
            for t in (base + core, base + 2 + core):
                wait_tile(t)
                forward(t).start()
            for t in (base + 1 - core, base + 3 - core):
                wait_tile(t)

        @pl.when(on_source_chip & jnp.logical_not(is_source))
        def _():
            for t in range(base, base + 4):
                wait_tile(t)

        block_of(theirs, theirs_e)(i, 0)

    table_copy.wait()
    for m in range(8):
        theirs_p[m] = theirs_e[within(tab[1, m], 7)]
    for copy in load_contrib:
        copy.wait()

    def update(s):
        rows = slice(s * size, (s + 1) * size)
        for q in range(16):
            left[q] = rows_v[within(tab[0, q], 15), rows]

        def two_cols(n, _):
            product = nt(
                left[...].reshape(16 * size, 1024), theirs_p[pl.ds(n * 2, 2)].reshape(256, 1024)
            )
            for t in range(2):
                for q in range(16):
                    tile = contrib_v[within(tab[1, 2 * n + t], 7), within(tab[0, q], 15), rows].astype(F32)
                    part = product[q * size : (q + 1) * size, t * TILE : (t + 1) * TILE]
                    packed[s, (q // 4) * 8 + 2 * n + t, q % 4] = (tile - part).astype(BF16)
            return 0

        lax.fori_loop(0, 4, two_cols, 0)

    def first_send(s):
        def send(t, _):
            _, row2, col2 = peer_of(front, z, core, x, (t * ORDER1) & 31)
            pltpu.make_async_remote_copy(
                src_ref=packed.at[s, row2 * 8 + col2], dst_ref=spread[s].at[here],
                send_sem=s1.at[s], recv_sem=r1.at[s],
                device_id=(front, row2, col2), device_id_type=MESH,
            ).start()
            return 0

        lax.fori_loop(1, 32, send, 0)
        spread[s][here] = packed[s, here]

    def first_all(s):
        return pltpu.make_async_remote_copy(
            src_ref=packed.at[s, pl.ds(0, 31)], dst_ref=spread[s].at[pl.ds(0, 31)],
            send_sem=s1.at[s], recv_sem=r1.at[s],
            device_id=(front, row, col), device_id_type=MESH,
        )

    def second_peer(t):
        return peer_of(front, z, core, x, (t * ORDER2) & 127)

    def second_copy(s, t):
        return pltpu.make_async_remote_copy(
            src_ref=ordered.at[s, t], dst_ref=landed[s].at[everywhere],
            send_sem=s2.at[s], recv_sem=r2.at[s],
            device_id=second_peer(t), device_id_type=MESH,
        )

    def second_send(s):
        def fill(t):
            f2, row2, col2 = second_peer(t)
            g = f2 * 4 + row2
            ordered[s, t] = spread[s][within(tab[2, g] + tab[3, col2], 31), within(tab[6, g], 3)]

        for t in range(GROUP):
            fill(t)
        landed[s][everywhere] = ordered[s, 0]
        for t in range(1, GROUP):
            second_copy(s, t).start()

        def step(i, _):
            for t in range(GROUP):
                fill(i * GROUP + t)
            for t in range(GROUP):
                second_copy(s, i * GROUP + t).start()
            return 0

        lax.fori_loop(1, 128 // GROUP, step, 0)

    def second_all(s):
        return pltpu.make_async_remote_copy(
            src_ref=ordered.at[s, pl.ds(0, 127)], dst_ref=landed[s].at[pl.ds(0, 127)],
            send_sem=s2.at[s], recv_sem=r2.at[s],
            device_id=(front, row, col), device_id_type=MESH,
        )

    def strip(a, s):
        return pl.ds(a * TILE + s * size, size)

    def write(a, s):
        return pltpu.make_async_copy(schur_v.at[strip(a, s)], schur.at[strip(a, s)], osem.at[s, a])

    def assemble(s):
        def row_of_tiles(a, _):
            rows = pl.ds(pl.multiple_of(a * TILE + s * size, size), size)
            for b in range(10):
                cols = slice(b * TILE, (b + 1) * TILE)
                total = init_v[rows, cols].astype(F32)
                for f in range(4):
                    m, k = tab[4, f * 5 + a], tab[5, f * 10 + b]
                    at = f * 32 + jnp.maximum(m - 1, 0) * 8 + jnp.maximum(k - 1, 0)
                    total = total + jnp.where((m > 0) & (k > 0), landed[s][within(at, 127)].astype(F32), 0.0)
                schur_v[rows, cols] = total
                rounded[pl.ds(pl.multiple_of(a * size, size), size), cols] = total.astype(BF16)
            return 0

        lax.fori_loop(0, 5, row_of_tiles, 0)
        for a in range(5):
            write(a, s).start()
        partial[s] = (
            jnp.dot(rounded[...], vectors_v[...], preferred_element_type=F32)
            .astype(BF16)
            .reshape(5, units, UNIT, partial.shape[-1])
        )

    def product_copies(s):
        copies = []
        for a in range(5):
            for j in range(units):
                u = (a * TILE + s * size) // UNIT + j
                copies.append(
                    (
                        u // 5,
                        u % 5,
                        partial.at[s, a, j],
                        pltpu.make_async_remote_copy(
                            src_ref=partial.at[s, a, j], dst_ref=sums.at[col, u % 5],
                            send_sem=s3, recv_sem=r3,
                            device_id=(front, row, u // 5), device_id_type=MESH,
                        ),
                    )
                )
        return copies

    def product_send(s):
        for to, at, value, copy in product_copies(s):

            @pl.when(col != to)
            def _():
                copy.start()

            @pl.when(col == to)
            def _():
                sums[to, at] = value[...]

    def product_all():
        return pltpu.make_async_remote_copy(
            src_ref=sums.at[pl.ds(0, 7)], dst_ref=sums.at[pl.ds(0, 7)], send_sem=s3, recv_sem=r3,
            device_id=(front, row, col), device_id_type=MESH,
        )

    for s in range(PARTS):
        update(s)
        first_send(s)
    for s in range(PARTS):
        first_all(s).wait_recv()
        second_send(s)
    load_init.wait()
    load_vectors.wait()
    for s in range(PARTS):
        second_all(s).wait_recv()
        assemble(s)
        product_send(s)
    for s in range(PARTS):
        first_all(s).wait_send()
        second_all(s).wait_send()
    product_all().wait_recv()
    total = sums[0].astype(F32)
    for c in range(1, 8):
        total = total + sums[c].astype(F32)
    product[...] = total.reshape(product.shape)
    product_all().wait_send()
    for s in range(PARTS):
        for a in range(5):
            write(a, s).wait()

    @pl.when(is_source)
    def _():
        for copy in source_sends():
            copy.wait_send()

    @pl.when(jnp.logical_not(on_source_chip))
    def _():
        for i in range(4):
            forward(2 * i + core).wait_send()


def fronts(row_tiles, col_tiles, owner, pivot, border, contrib, inverse_set, init, vectors):
    hbm = pl.BlockSpec(memory_space=pl.ANY)
    vmem = pl.BlockSpec(memory_space=pltpu.VMEM)
    size = TILE // PARTS
    rows, cols = init.shape
    wide = vectors.shape[1]
    return pl.pallas_call(
        front_kernel,
        out_shape=(
            jax.ShapeDtypeStruct((rows, cols), F32),
            jax.ShapeDtypeStruct((rows // 8, wide), F32),
        ),
        in_specs=[vmem, vmem, vmem, hbm, hbm, hbm, vmem, hbm, hbm],
        out_specs=(hbm, vmem),
        scratch_shapes=[
            pltpu.VMEM((8, TILE), jnp.int32),
            pltpu.SMEM((8, TILE), jnp.int32),
            pltpu.VMEM((16, TILE, 1024), BF16),
            pltpu.VMEM((8, TILE, 1024), BF16),
            pltpu.VMEM((8, TILE, 1024), BF16),
            pltpu.VMEM((8, TILE, 1024), BF16),
            pltpu.VMEM((1024, 1024), BF16),
            pltpu.VMEM((8, 16, TILE, TILE), BF16),
            pltpu.VMEM((16, size, 1024), BF16),
            pltpu.VMEM((PARTS, 32, 4, size, TILE), BF16),
            pltpu.VMEM((PARTS, 128, size, TILE), BF16),
            pltpu.VMEM((rows, cols), BF16),
            pltpu.VMEM((cols, wide), BF16),
            pltpu.VMEM((rows, cols), F32),
            pltpu.VMEM((5 * size, cols), BF16),
            pltpu.VMEM((PARTS, 5, size // UNIT, UNIT, wide), BF16),
            pltpu.VMEM((8, 5, UNIT, wide), BF16),
            pltpu.SemaphoreType.DMA((16,)),
            pltpu.SemaphoreType.DMA((8,)),
            pltpu.SemaphoreType.DMA((21,)),
            *[pltpu.SemaphoreType.DMA((PARTS,))] * 4,
            pltpu.SemaphoreType.DMA((PARTS, 5)),
            pltpu.SemaphoreType.DMA,
            pltpu.SemaphoreType.DMA,
            *[pltpu.VMEM((32, 4, size, TILE), BF16)] * PARTS,
            *[pltpu.VMEM((128, size, TILE), BF16)] * PARTS,
        ],
        compiler_params=pltpu.CompilerParams(
            collective_id=0, has_side_effects=True, vmem_limit_bytes=60 << 20
        ),
        name="fronts",
    )(
        row_tiles, col_tiles, owner.reshape(1, owner.size), pivot, border.reshape(16, TILE, 1024),
        contrib.reshape(16, TILE, 1024), inverse_set, init, vectors,
    )


def shards(pivot_block, border, contrib, inverses, row_tiles, col_tiles, owner, schur_init, block):
    return fronts(
        row_tiles, col_tiles, owner, pivot_block, border, contrib, inverses, schur_init, block
    )


def solution(mesh):
    in_specs = (
        P("front", None, None),
        P("front", "row", None),
        P("front", "row", "col"),
        P("front", None, None, None),
        P(),
        P(),
        P(),
        P(("front", "row"), "col"),
        P("col", None),
    )
    out_specs = (P(("front", "row"), "col"), P(("front", "row", "col"), None))
    return jax.shard_map(shards, mesh=mesh, in_specs=in_specs, out_specs=out_specs, check_vma=False)
```

```python
import functools

import jax
import jax.numpy as jnp
from jax import lax
from jax.experimental import pallas as pl
from jax.experimental.pallas import tpu as pltpu
from jax.sharding import PartitionSpec as P

TILE = 128
MESH = pl.DeviceIdType.MESH
F32 = jnp.float32
BF16 = jnp.bfloat16


def within(index, last):
    return jnp.minimum(jnp.maximum(index, 0), last)


def nt(a, b):
    return lax.dot_general(a, b, (((1,), (1,)), ((), ())), preferred_element_type=F32)


def split_levels(src_c, src_r, dst_c, dst_r, squarings):
    n = src_c.shape[0]
    at_c = lax.broadcasted_iota(jnp.int32, (n, n), 0).astype(F32)
    at_r = lax.broadcasted_iota(jnp.int32, (n, n), 1).astype(F32)
    color_c = jnp.zeros((n, 1), F32)
    color_r = jnp.zeros((1, n), F32)

    def partners(node_c, node_r):
        same = jnp.where((node_c == node_r) & (color_c == color_r), 1.0, 0.0)
        rank_c = jnp.sum(jnp.where(at_r < at_c, same, 0.0), axis=1, keepdims=True)
        rank_r = jnp.sum(jnp.where(at_c < at_r, same, 0.0), axis=0, keepdims=True)
        pair = (jnp.floor(rank_c * 0.5) == jnp.floor(rank_r * 0.5)) & (at_c != at_r)
        return jnp.where(pair, same, 0.0)

    for count in squarings:
        by_src = partners(src_c, src_r)
        by_dst = partners(dst_c, dst_r)
        reach = jnp.dot(by_src.astype(BF16), by_dst.astype(BF16), preferred_element_type=F32)
        reach = jnp.where(at_c == at_r, 1.0, reach)
        for _ in range(count):
            half = reach.astype(BF16)
            reach = jnp.where(jnp.dot(half, half, preferred_element_type=F32) > 0.5, 1.0, 0.0)
        far = float(n)
        label_c = jnp.min(jnp.where(reach > 0.5, at_r, far), axis=1, keepdims=True)
        label_r = jnp.min(jnp.where(reach > 0.5, at_c, far), axis=0, keepdims=True)
        other_c = jnp.sum(by_src * label_r, axis=1, keepdims=True)
        other_r = jnp.sum(by_src * label_c, axis=0, keepdims=True)
        color_c = color_c * 2.0 + jnp.where(label_c > other_c, 1.0, 0.0)
        color_r = color_r * 2.0 + jnp.where(label_r > other_r, 1.0, 0.0)
    return color_c


TABLE_ROWS = ((16, 15), (8, 7), (16, 24), (8, 7), (20, 4), (40, 8), (16, 3))


def div(x, by):
    return jnp.floor((x + 0.5) * (1.0 / by))


def routing(rows_c, rows_r, cols_c, cols_r, owner_r, owner_c, front, row, col):
    n = rows_c.shape[0]
    per = n // 4
    slots = owner_r.shape[1]
    lane = lax.broadcasted_iota(jnp.int32, (n, slots), 1)
    sub = lax.broadcasted_iota(jnp.int32, (slots, n), 0)
    own_r = owner_r.astype(F32)
    own_c = owner_c.astype(F32)

    def slot_c(ids):
        return jnp.sum(jnp.where(ids == lane, own_r, 0.0), axis=1, keepdims=True)

    def slot_r(ids):
        return jnp.sum(jnp.where(ids == sub, own_c, 0.0), axis=0, keepdims=True)

    e_c = lax.broadcasted_iota(jnp.int32, (n, 1), 0).astype(F32)
    e_r = lax.broadcasted_iota(jnp.int32, (1, n), 1).astype(F32)
    f_c, f_r = div(e_c, per), div(e_r, per)
    i_c = e_c - f_c * per
    rs_c, rs_r, cs_c, cs_r = slot_c(rows_c), slot_r(rows_r), slot_c(cols_c), slot_r(cols_r)
    g_c, g_r, h_c, h_r = div(rs_c, 5), div(rs_r, 5), div(cs_c, 10), div(cs_r, 10)
    a_c, b_c = rs_c - g_c * 5, cs_c - h_c * 10
    mr = split_levels(div(e_c, 4), div(e_r, 4), f_c * 16 + g_c, f_r * 16 + g_r, (5, 4))
    mc = split_levels(div(e_c, 8), div(e_r, 8), f_c * 8 + h_c, f_r * 8 + h_r, (5, 4, 3))
    front, row, col = front.astype(F32), row.astype(F32), col.astype(F32)
    mine = f_c == front
    q = lax.broadcasted_iota(jnp.int32, (n, TILE), 1).astype(F32)

    def table(mask, value):
        return jnp.sum(jnp.where(mask, value, 0.0), axis=0, keepdims=True)

    in_row = i_c - div(i_c, 16) * 16
    chunk = div(in_row, 4)
    t0 = table(mine & (div(i_c, 16) == row) & (mr * 4 + chunk == q), in_row)
    block = div(i_c, 8)
    t1 = table(mine & (block == col) & (mc == q), i_c - block * 8)
    at_row = mine & (mr == row) & (g_c == q)
    t2 = table(at_row, div(i_c, 16) * 8)
    t3 = table(mine & (mc == col) & (h_c == q), block)
    t6 = table(at_row, chunk)
    t4 = table((g_c == front * 4 + row) & (f_c * 5 + a_c == q), mr + 1.0)
    t5 = table((h_c == col) & (f_c * 10 + b_c == q), mc + 1.0)
    zero = jnp.zeros_like(t0)
    tops = (15.0, 7.0, 24.0, 7.0, 4.0, 8.0, 3.0, 0.0)
    tables = [jnp.minimum(t, top) for t, top in zip((t0, t1, t2, t3, t4, t5, t6, zero), tops)]
    return jnp.concatenate(tables, axis=0).astype(jnp.int32)


def both_ways(ids):
    fronts, per = ids.shape
    n = fronts * per
    spread = jnp.where(
        lax.broadcasted_iota(jnp.int32, (per, n), 0) == lax.broadcasted_iota(jnp.int32, (per, n), 1) % per, 1.0, 0.0
    )
    wide = jnp.dot(ids.astype(F32).astype(BF16), spread.astype(BF16), preferred_element_type=F32)
    here = lax.broadcasted_iota(jnp.int32, (fronts, n), 0) == lax.broadcasted_iota(jnp.int32, (fronts, n), 1) // per
    flat = jnp.sum(jnp.where(here, wide, 0.0), axis=0, keepdims=True)
    return turned(flat).astype(jnp.int32), flat.astype(jnp.int32)


def turned(flat):
    n = flat.shape[1]
    eye = lax.broadcasted_iota(jnp.int32, (n, n), 0) == lax.broadcasted_iota(jnp.int32, (n, n), 1)
    return jnp.sum(jnp.where(eye, flat, 0.0), axis=1, keepdims=True)


def position():
    front, row, col = lax.axis_index("front"), lax.axis_index("row"), lax.axis_index("col")
    return front, row // 2, row % 2, col // 2, col % 2


def device(front, z, core, x):
    return (front, (z % 2) * 2 + core, x * 2 + z // 2)


def eliminate_rows(block, lower, inverse_set):
    parts = []
    for k in range(4):
        now = block[:, k * 256 : (k + 1) * 256].astype(F32)
        for j in range(k):
            now = now - nt(parts[j], lower[k * 256 : (k + 1) * 256, j * 256 : (j + 1) * 256])
        parts.append(
            jnp.dot(now.astype(BF16), inverse_set[k], preferred_element_type=F32).astype(BF16)
        )
    return parts


PARTS = 8


ORDER1 = 11
ORDER2 = 37


def peer_of(front, z, core, x, u):
    dk, dx, dz, dy = u & 1, (u >> 1) & 3, (u >> 3) & 3, u >> 5
    f2, z2, k2, x2 = (front + dy) & 3, (z + dz) & 3, core ^ dk, (x + dx) & 3
    return f2, ((z2 & 1) << 1) + k2, (x2 << 1) + (z2 >> 1)


GROUP = 8
UNIT = 16


def front_kernel(
    row_tiles, col_tiles, owner, pivot, border, contrib, inverse_set, init, vectors, schur, product,
    tab_v, tab_raw, tab, rows_v, theirs, theirs_e, theirs_p, lower, contrib_v, left, packed, ordered, init_v, vectors_v, schur_v,
    rounded, partial, sums, bsend, brecv, lsem, s1, r1, s2, r2, osem, s3, r3, *buffers,
):
    spread, landed = buffers[:PARTS], buffers[PARTS:]
    size = TILE // PARTS
    units = size // UNIT
    front, z_lo, core, x, z_hi = position()
    z = z_hi * 2 + z_lo
    row, col = lax.axis_index("row"), lax.axis_index("col")
    here = row * 8 + col
    everywhere = front * 32 + here
    up, down = (z + 1) & 3, (z + 3) & 3
    on_source_chip = z_lo == x // 2
    is_source = on_source_chip & (core == x % 2)
    sibling = device(front, z, 1 - core, x)
    barrier = pltpu.get_barrier_semaphore()

    def greet(u, _):
        pl.semaphore_signal(barrier, inc=1, device_id=peer_of(front, z, core, x, u), device_id_type=MESH)
        return 0

    lax.fori_loop(1, 128, greet, 0)
    load_lower = pltpu.make_async_copy(pivot.at[0], lower, lsem.at[0])
    load_rows = pltpu.make_async_copy(border, rows_v, lsem.at[1])
    load_init = pltpu.make_async_copy(init, init_v, lsem.at[2])
    load_vectors = pltpu.make_async_copy(vectors, vectors_v, lsem.at[3])
    load_contrib = [
        pltpu.make_async_copy(
            contrib.at[:, :, j * TILE : (j + 1) * TILE], contrib_v.at[j], lsem.at[4 + j]
        )
        for j in range(8)
    ]
    load_lower.start()
    load_rows.start()
    pl.semaphore_wait(barrier, 127)

    def push(src, tile, sem, peer):
        return pltpu.make_async_remote_copy(
            src_ref=src, dst_ref=theirs.at[tile], send_sem=bsend.at[sem], recv_sem=brecv.at[tile],
            device_id=peer, device_id_type=MESH,
        )

    def source_sends():
        sends = []
        for tile in (0, 2, 1, 3, 4, 6, 5, 7):
            to = down if tile & 2 else up
            sends.append(push(border.at[(to >> 1) * 8 + tile], tile, tile, device(front, to, tile & 1, x)))
        for tile in range(8):
            sends.append(push(border.at[z_hi * 8 + tile], tile, 8 + tile, sibling))
        return sends

    def own_tiles(first, last):
        return [
            pltpu.make_async_copy(border.at[z_hi * 8 + t], theirs.at[t], lsem.at[12 + t]) for t in range(first, last)
        ]

    @pl.when(is_source)
    def _():
        for copy in source_sends():
            copy.start()
        for copy in own_tiles(0, 8):
            copy.start()

    for copy in load_contrib:
        copy.start()
    load_init.start()
    load_vectors.start()
    rows_c, rows_r = both_ways(row_tiles[...])
    cols_c, cols_r = both_ways(col_tiles[...])
    tab_v[...] = routing(
        rows_c, rows_r, cols_c, cols_r, owner[...], turned(owner[...].astype(F32)), front, row, col
    )
    load_lower.wait()
    for k in range(3):
        low = (k + 1) * 256
        now = lower[low:, k * 256 : (k + 1) * 256].astype(F32)
        for j in range(k):
            now = now - nt(
                lower[low:, j * 256 : (j + 1) * 256], lower[k * 256 : low, j * 256 : (j + 1) * 256]
            )
        lower[low:, k * 256 : (k + 1) * 256] = jnp.dot(
            now.astype(BF16), inverse_set[0, k], preferred_element_type=F32
        ).astype(BF16)
    load_rows.wait()

    def block_of(source, target):
        def step(i, _):
            rows = pl.ds(i * 4, 4)
            parts = eliminate_rows(source[rows].reshape(512, 1024), lower, inverse_set.at[0])
            for k in range(4):
                target[rows, :, k * 256 : (k + 1) * 256] = parts[k].reshape(4, TILE, 256)
            return 0

        return step

    lax.fori_loop(0, 4, block_of(rows_v, rows_v), 0)
    table_copy = pltpu.make_async_copy(tab_v, tab_raw, lsem.at[20])
    table_copy.start()

    def wait_tile(t):
        push(theirs.at[t], t, 0, sibling).wait_recv()

    def forward(t):
        return push(theirs.at[t], t, t >> 1, sibling)

    for i in range(2):
        base = 4 * i

        @pl.when(is_source)
        def _():
            for copy in own_tiles(base, base + 4):
                copy.wait()

        @pl.when(jnp.logical_not(on_source_chip))
        def _():
            for t in (base + core, base + 2 + core):
                wait_tile(t)
                forward(t).start()
            for t in (base + 1 - core, base + 3 - core):
                wait_tile(t)

        @pl.when(on_source_chip & jnp.logical_not(is_source))
        def _():
            for t in range(base, base + 4):
                wait_tile(t)

        block_of(theirs, theirs_e)(i, 0)

    table_copy.wait()
    for r, (count, last) in enumerate(TABLE_ROWS):
        for at in range(count):
            tab[r, at] = within(tab_raw[r, at], last)
    for m in range(8):
        theirs_p[m] = theirs_e[tab[1, m]]
    for copy in load_contrib:
        copy.wait()

    def update(s):
        rows = slice(s * size, (s + 1) * size)
        for q in range(16):
            left[q] = rows_v[tab[0, q], rows]

        def two_cols(n, _):
            product = nt(
                left[...].reshape(16 * size, 1024), theirs_p[pl.ds(n * 2, 2)].reshape(256, 1024)
            )
            for t in range(2):
                for q in range(16):
                    tile = contrib_v[tab[1, 2 * n + t], tab[0, q], rows].astype(F32)
                    part = product[q * size : (q + 1) * size, t * TILE : (t + 1) * TILE]
                    packed[s, (q // 4) * 8 + 2 * n + t, q % 4] = (tile - part).astype(BF16)
            return 0

        lax.fori_loop(0, 4, two_cols, 0)

    def first_send(s):
        def send(t, _):
            _, row2, col2 = peer_of(front, z, core, x, (t * ORDER1) & 31)
            pltpu.make_async_remote_copy(
                src_ref=packed.at[s, row2 * 8 + col2], dst_ref=spread[s].at[here],
                send_sem=s1.at[s], recv_sem=r1.at[s],
                device_id=(front, row2, col2), device_id_type=MESH,
            ).start()
            return 0

        lax.fori_loop(1, 32, send, 0)
        spread[s][here] = packed[s, here]

    def first_all(s):
        return pltpu.make_async_remote_copy(
            src_ref=packed.at[s, pl.ds(0, 31)], dst_ref=spread[s].at[pl.ds(0, 31)],
            send_sem=s1.at[s], recv_sem=r1.at[s],
            device_id=(front, row, col), device_id_type=MESH,
        )

    def second_peer(t):
        return peer_of(front, z, core, x, (t * ORDER2) & 127)

    def second_copy(s, t):
        return pltpu.make_async_remote_copy(
            src_ref=ordered.at[s, t], dst_ref=landed[s].at[everywhere],
            send_sem=s2.at[s], recv_sem=r2.at[s],
            device_id=second_peer(t), device_id_type=MESH,
        )

    def second_send(s):
        def fill(t):
            f2, row2, col2 = second_peer(t)
            g = f2 * 4 + row2
            ordered[s, t] = spread[s][tab[2, g] + tab[3, col2], tab[6, g]]

        for t in range(GROUP):
            fill(t)
        landed[s][everywhere] = ordered[s, 0]
        for t in range(1, GROUP):
            second_copy(s, t).start()

        def step(i, _):
            for t in range(GROUP):
                fill(i * GROUP + t)
            for t in range(GROUP):
                second_copy(s, i * GROUP + t).start()
            return 0

        lax.fori_loop(1, 128 // GROUP, step, 0)

    def second_all(s):
        return pltpu.make_async_remote_copy(
            src_ref=ordered.at[s, pl.ds(0, 127)], dst_ref=landed[s].at[pl.ds(0, 127)],
            send_sem=s2.at[s], recv_sem=r2.at[s],
            device_id=(front, row, col), device_id_type=MESH,
        )

    def strip(a, s):
        return pl.ds(a * TILE + s * size, size)

    def write(a, s):
        return pltpu.make_async_copy(schur_v.at[strip(a, s)], schur.at[strip(a, s)], osem.at[s, a])

    def assemble(s):
        def row_of_tiles(a, _):
            rows = pl.ds(pl.multiple_of(a * TILE + s * size, size), size)
            for b in range(10):
                cols = slice(b * TILE, (b + 1) * TILE)
                total = init_v[rows, cols].astype(F32)
                for f in range(4):
                    m, k = tab[4, f * 5 + a], tab[5, f * 10 + b]
                    at = f * 32 + jnp.maximum(m - 1, 0) * 8 + jnp.maximum(k - 1, 0)
                    total = total + jnp.where((m > 0) & (k > 0), landed[s][at].astype(F32), 0.0)
                schur_v[rows, cols] = total
                rounded[pl.ds(pl.multiple_of(a * size, size), size), cols] = total.astype(BF16)
            return 0

        lax.fori_loop(0, 5, row_of_tiles, 0)
        for a in range(5):
            write(a, s).start()
        partial[s] = (
            jnp.dot(rounded[...], vectors_v[...], preferred_element_type=F32)
            .astype(BF16)
            .reshape(5, units, UNIT, partial.shape[-1])
        )

    def product_copies(s):
        copies = []
        for a in range(5):
            for j in range(units):
                u = (a * TILE + s * size) // UNIT + j
                copies.append(
                    (
                        u // 5,
                        u % 5,
                        partial.at[s, a, j],
                        pltpu.make_async_remote_copy(
                            src_ref=partial.at[s, a, j], dst_ref=sums.at[col, u % 5],
                            send_sem=s3, recv_sem=r3,
                            device_id=(front, row, u // 5), device_id_type=MESH,
                        ),
                    )
                )
        return copies

    def product_send(s):
        for to, at, value, copy in product_copies(s):

            @pl.when(col != to)
            def _():
                copy.start()

            @pl.when(col == to)
            def _():
                sums[to, at] = value[...]

    def product_all():
        return pltpu.make_async_remote_copy(
            src_ref=sums.at[pl.ds(0, 7)], dst_ref=sums.at[pl.ds(0, 7)], send_sem=s3, recv_sem=r3,
            device_id=(front, row, col), device_id_type=MESH,
        )

    for s in range(PARTS):
        update(s)
        first_send(s)
    for s in range(PARTS):
        first_all(s).wait_recv()
        second_send(s)
    load_init.wait()
    load_vectors.wait()
    for s in range(PARTS):
        second_all(s).wait_recv()
        assemble(s)
        product_send(s)
    for s in range(PARTS):
        first_all(s).wait_send()
        second_all(s).wait_send()
    product_all().wait_recv()
    total = sums[0].astype(F32)
    for c in range(1, 8):
        total = total + sums[c].astype(F32)
    product[...] = total.reshape(product.shape)
    product_all().wait_send()
    for s in range(PARTS):
        for a in range(5):
            write(a, s).wait()

    @pl.when(is_source)
    def _():
        for copy in source_sends():
            copy.wait_send()

    @pl.when(jnp.logical_not(on_source_chip))
    def _():
        for i in range(4):
            forward(2 * i + core).wait_send()


def fronts(row_tiles, col_tiles, owner, pivot, border, contrib, inverse_set, init, vectors):
    hbm = pl.BlockSpec(memory_space=pl.ANY)
    vmem = pl.BlockSpec(memory_space=pltpu.VMEM)
    size = TILE // PARTS
    rows, cols = init.shape
    wide = vectors.shape[1]
    return pl.pallas_call(
        front_kernel,
        out_shape=(
            jax.ShapeDtypeStruct((rows, cols), F32),
            jax.ShapeDtypeStruct((rows // 8, wide), F32),
        ),
        in_specs=[vmem, vmem, vmem, hbm, hbm, hbm, vmem, hbm, hbm],
        out_specs=(hbm, vmem),
        scratch_shapes=[
            pltpu.VMEM((8, TILE), jnp.int32),
            pltpu.SMEM((8, TILE), jnp.int32),
            pltpu.SMEM((8, TILE), jnp.int32),
            pltpu.VMEM((16, TILE, 1024), BF16),
            pltpu.VMEM((8, TILE, 1024), BF16),
            pltpu.VMEM((8, TILE, 1024), BF16),
            pltpu.VMEM((8, TILE, 1024), BF16),
            pltpu.VMEM((1024, 1024), BF16),
            pltpu.VMEM((8, 16, TILE, TILE), BF16),
            pltpu.VMEM((16, size, 1024), BF16),
            pltpu.VMEM((PARTS, 32, 4, size, TILE), BF16),
            pltpu.VMEM((PARTS, 128, size, TILE), BF16),
            pltpu.VMEM((rows, cols), BF16),
            pltpu.VMEM((cols, wide), BF16),
            pltpu.VMEM((rows, cols), F32),
            pltpu.VMEM((5 * size, cols), BF16),
            pltpu.VMEM((PARTS, 5, size // UNIT, UNIT, wide), BF16),
            pltpu.VMEM((8, 5, UNIT, wide), BF16),
            pltpu.SemaphoreType.DMA((16,)),
            pltpu.SemaphoreType.DMA((8,)),
            pltpu.SemaphoreType.DMA((21,)),
            *[pltpu.SemaphoreType.DMA((PARTS,))] * 4,
            pltpu.SemaphoreType.DMA((PARTS, 5)),
            pltpu.SemaphoreType.DMA,
            pltpu.SemaphoreType.DMA,
            *[pltpu.VMEM((32, 4, size, TILE), BF16)] * PARTS,
            *[pltpu.VMEM((128, size, TILE), BF16)] * PARTS,
        ],
        compiler_params=pltpu.CompilerParams(
            collective_id=0, has_side_effects=True, vmem_limit_bytes=60 << 20
        ),
        name="fronts",
    )(
        row_tiles, col_tiles, owner.reshape(1, owner.size), pivot, border.reshape(16, TILE, 1024),
        contrib.reshape(16, TILE, 1024), inverse_set, init, vectors,
    )


def shards(pivot_block, border, contrib, inverses, row_tiles, col_tiles, owner, schur_init, block):
    return fronts(
        row_tiles, col_tiles, owner, pivot_block, border, contrib, inverses, schur_init, block
    )


def solution(mesh):
    in_specs = (
        P("front", None, None),
        P("front", "row", None),
        P("front", "row", "col"),
        P("front", None, None, None),
        P(),
        P(),
        P(),
        P(("front", "row"), "col"),
        P("col", None),
    )
    out_specs = (P(("front", "row"), "col"), P(("front", "row", "col"), None))
    return jax.shard_map(shards, mesh=mesh, in_specs=in_specs, out_specs=out_specs, check_vma=False)
```

```python
import functools

import jax
import jax.numpy as jnp
from jax import lax
from jax.experimental import pallas as pl
from jax.experimental.pallas import tpu as pltpu
from jax.sharding import PartitionSpec as P

TILE = 128
MESH = pl.DeviceIdType.MESH
F32 = jnp.float32
BF16 = jnp.bfloat16


def within(index, last):
    return jnp.minimum(jnp.maximum(index, 0), last)


def nt(a, b):
    return lax.dot_general(a, b, (((1,), (1,)), ((), ())), preferred_element_type=F32)


def split_levels(src_c, src_r, dst_c, dst_r, squarings):
    n = src_c.shape[0]
    at_c = lax.broadcasted_iota(jnp.int32, (n, n), 0).astype(F32)
    at_r = lax.broadcasted_iota(jnp.int32, (n, n), 1).astype(F32)
    color_c = jnp.zeros((n, 1), F32)
    color_r = jnp.zeros((1, n), F32)

    def partners(node_c, node_r):
        same = jnp.where((node_c == node_r) & (color_c == color_r), 1.0, 0.0)
        rank_c = jnp.sum(jnp.where(at_r < at_c, same, 0.0), axis=1, keepdims=True)
        rank_r = jnp.sum(jnp.where(at_c < at_r, same, 0.0), axis=0, keepdims=True)
        pair = (jnp.floor(rank_c * 0.5) == jnp.floor(rank_r * 0.5)) & (at_c != at_r)
        return jnp.where(pair, same, 0.0)

    for count in squarings:
        by_src = partners(src_c, src_r)
        by_dst = partners(dst_c, dst_r)
        reach = jnp.dot(by_src.astype(BF16), by_dst.astype(BF16), preferred_element_type=F32)
        reach = jnp.where(at_c == at_r, 1.0, reach)
        for _ in range(count):
            half = reach.astype(BF16)
            reach = jnp.where(jnp.dot(half, half, preferred_element_type=F32) > 0.5, 1.0, 0.0)
        far = float(n)
        label_c = jnp.min(jnp.where(reach > 0.5, at_r, far), axis=1, keepdims=True)
        label_r = jnp.min(jnp.where(reach > 0.5, at_c, far), axis=0, keepdims=True)
        other_c = jnp.sum(by_src * label_r, axis=1, keepdims=True)
        other_r = jnp.sum(by_src * label_c, axis=0, keepdims=True)
        color_c = color_c * 2.0 + jnp.where(label_c > other_c, 1.0, 0.0)
        color_r = color_r * 2.0 + jnp.where(label_r > other_r, 1.0, 0.0)
    return color_c


TABLE_ROWS = ((16, 15), (8, 7), (16, 24), (8, 7), (20, 4), (40, 8), (16, 3))


def div(x, by):
    return jnp.floor((x + 0.5) * (1.0 / by))


def routing(rows_c, rows_r, cols_c, cols_r, owner_r, owner_c, front, row, col):
    n = rows_c.shape[0]
    per = n // 4
    slots = owner_r.shape[1]
    lane = lax.broadcasted_iota(jnp.int32, (n, slots), 1)
    sub = lax.broadcasted_iota(jnp.int32, (slots, n), 0)
    own_r = owner_r.astype(F32)
    own_c = owner_c.astype(F32)

    def slot_c(ids):
        return jnp.sum(jnp.where(ids == lane, own_r, 0.0), axis=1, keepdims=True)

    def slot_r(ids):
        return jnp.sum(jnp.where(ids == sub, own_c, 0.0), axis=0, keepdims=True)

    e_c = lax.broadcasted_iota(jnp.int32, (n, 1), 0).astype(F32)
    e_r = lax.broadcasted_iota(jnp.int32, (1, n), 1).astype(F32)
    f_c, f_r = div(e_c, per), div(e_r, per)
    i_c = e_c - f_c * per
    rs_c, rs_r, cs_c, cs_r = slot_c(rows_c), slot_r(rows_r), slot_c(cols_c), slot_r(cols_r)
    g_c, g_r, h_c, h_r = div(rs_c, 5), div(rs_r, 5), div(cs_c, 10), div(cs_r, 10)
    a_c, b_c = rs_c - g_c * 5, cs_c - h_c * 10
    mr = split_levels(div(e_c, 4), div(e_r, 4), f_c * 16 + g_c, f_r * 16 + g_r, (5, 4))
    mc = split_levels(div(e_c, 8), div(e_r, 8), f_c * 8 + h_c, f_r * 8 + h_r, (5, 4, 3))
    front, row, col = front.astype(F32), row.astype(F32), col.astype(F32)
    mine = f_c == front
    q = lax.broadcasted_iota(jnp.int32, (n, TILE), 1).astype(F32)

    def table(mask, value):
        return jnp.sum(jnp.where(mask, value, 0.0), axis=0, keepdims=True)

    in_row = i_c - div(i_c, 16) * 16
    chunk = div(in_row, 4)
    t0 = table(mine & (div(i_c, 16) == row) & (mr * 4 + chunk == q), in_row)
    block = div(i_c, 8)
    t1 = table(mine & (block == col) & (mc == q), i_c - block * 8)
    at_row = mine & (mr == row) & (g_c == q)
    t2 = table(at_row, div(i_c, 16) * 8)
    t3 = table(mine & (mc == col) & (h_c == q), block)
    t6 = table(at_row, chunk)
    t4 = table((g_c == front * 4 + row) & (f_c * 5 + a_c == q), mr + 1.0)
    t5 = table((h_c == col) & (f_c * 10 + b_c == q), mc + 1.0)
    zero = jnp.zeros_like(t0)
    tops = (15.0, 7.0, 24.0, 7.0, 4.0, 8.0, 3.0, 0.0)
    tables = [jnp.minimum(t, top) for t, top in zip((t0, t1, t2, t3, t4, t5, t6, zero), tops)]
    return jnp.concatenate(tables, axis=0).astype(jnp.int32)


def both_ways(ids):
    fronts, per = ids.shape
    n = fronts * per
    spread = jnp.where(
        lax.broadcasted_iota(jnp.int32, (per, n), 0) == lax.broadcasted_iota(jnp.int32, (per, n), 1) % per, 1.0, 0.0
    )
    wide = jnp.dot(ids.astype(F32).astype(BF16), spread.astype(BF16), preferred_element_type=F32)
    here = lax.broadcasted_iota(jnp.int32, (fronts, n), 0) == lax.broadcasted_iota(jnp.int32, (fronts, n), 1) // per
    flat = jnp.sum(jnp.where(here, wide, 0.0), axis=0, keepdims=True)
    return turned(flat).astype(jnp.int32), flat.astype(jnp.int32)


def turned(flat):
    n = flat.shape[1]
    eye = lax.broadcasted_iota(jnp.int32, (n, n), 0) == lax.broadcasted_iota(jnp.int32, (n, n), 1)
    return jnp.sum(jnp.where(eye, flat, 0.0), axis=1, keepdims=True)


def position():
    front, row, col = lax.axis_index("front"), lax.axis_index("row"), lax.axis_index("col")
    return front, row // 2, row % 2, col // 2, col % 2


def device(front, z, core, x):
    return (front, (z % 2) * 2 + core, x * 2 + z // 2)


def eliminate_rows(block, lower, inverse_set):
    parts = []
    for k in range(4):
        now = block[:, k * 256 : (k + 1) * 256].astype(F32)
        for j in range(k):
            now = now - nt(parts[j], lower[k * 256 : (k + 1) * 256, j * 256 : (j + 1) * 256])
        parts.append(
            jnp.dot(now.astype(BF16), inverse_set[k], preferred_element_type=F32).astype(BF16)
        )
    return parts


PARTS = 8


ORDER1 = 11
ORDER2 = 37


def peer_of(front, z, core, x, u):
    dk, dx, dz, dy = u & 1, (u >> 1) & 3, (u >> 3) & 3, u >> 5
    f2, z2, k2, x2 = (front + dy) & 3, (z + dz) & 3, core ^ dk, (x + dx) & 3
    return f2, ((z2 & 1) << 1) + k2, (x2 << 1) + (z2 >> 1)


GROUP = 8
UNIT = 16


def front_kernel(
    row_tiles, col_tiles, owner, pivot, border, contrib, inverse_set, init, vectors, schur, product,
    tab_v, tab_raw, tab, rows_v, theirs, theirs_e, theirs_p, lower, contrib_v, left, packed, ordered, init_v, vectors_v, schur_v,
    rounded, partial, sums, bsend, brecv, lsem, s1, r1, s2, r2, osem, s3, r3, *buffers,
):
    spread, landed = buffers[:PARTS], buffers[PARTS:]
    size = TILE // PARTS
    units = size // UNIT
    front, z_lo, core, x, z_hi = position()
    z = z_hi * 2 + z_lo
    row, col = lax.axis_index("row"), lax.axis_index("col")
    here = row * 8 + col
    everywhere = front * 32 + here
    up, down = (z + 1) & 3, (z + 3) & 3
    on_source_chip = z_lo == x // 2
    is_source = on_source_chip & (core == x % 2)
    sibling = device(front, z, 1 - core, x)
    barrier = pltpu.get_barrier_semaphore()

    def greet(u, _):
        pl.semaphore_signal(barrier, inc=1, device_id=peer_of(front, z, core, x, u), device_id_type=MESH)
        return 0

    lax.fori_loop(1, 128, greet, 0)
    load_lower = pltpu.make_async_copy(pivot.at[0], lower, lsem.at[0])
    load_rows = pltpu.make_async_copy(border, rows_v, lsem.at[1])
    load_init = pltpu.make_async_copy(init, init_v, lsem.at[2])
    load_vectors = pltpu.make_async_copy(vectors, vectors_v, lsem.at[3])
    load_contrib = [
        pltpu.make_async_copy(
            contrib.at[:, :, j * TILE : (j + 1) * TILE], contrib_v.at[j], lsem.at[4 + j]
        )
        for j in range(8)
    ]
    load_lower.start()
    load_rows.start()
    pl.semaphore_wait(barrier, 127)

    def push(src, tile, sem, peer):
        return pltpu.make_async_remote_copy(
            src_ref=src, dst_ref=theirs.at[tile], send_sem=bsend.at[sem], recv_sem=brecv.at[tile],
            device_id=peer, device_id_type=MESH,
        )

    def source_sends():
        sends = []
        for tile in (0, 2, 1, 3, 4, 6, 5, 7):
            to = down if tile & 2 else up
            sends.append(push(border.at[(to >> 1) * 8 + tile], tile, tile, device(front, to, tile & 1, x)))
        for tile in range(8):
            sends.append(push(border.at[z_hi * 8 + tile], tile, 8 + tile, sibling))
        return sends

    def own_tiles(first, last):
        return [
            pltpu.make_async_copy(border.at[z_hi * 8 + t], theirs.at[t], lsem.at[12 + t]) for t in range(first, last)
        ]

    @pl.when(is_source)
    def _():
        for copy in source_sends():
            copy.start()
        for copy in own_tiles(0, 8):
            copy.start()

    for copy in load_contrib:
        copy.start()
    load_init.start()
    load_vectors.start()
    rows_c, rows_r = both_ways(row_tiles[...])
    cols_c, cols_r = both_ways(col_tiles[...])
    tab_v[...] = routing(
        rows_c, rows_r, cols_c, cols_r, owner[...], turned(owner[...].astype(F32)), front, row, col
    )
    load_lower.wait()
    for k in range(3):
        low = (k + 1) * 256
        now = lower[low:, k * 256 : (k + 1) * 256].astype(F32)
        for j in range(k):
            now = now - nt(
                lower[low:, j * 256 : (j + 1) * 256], lower[k * 256 : low, j * 256 : (j + 1) * 256]
            )
        lower[low:, k * 256 : (k + 1) * 256] = jnp.dot(
            now.astype(BF16), inverse_set[0, k], preferred_element_type=F32
        ).astype(BF16)
    load_rows.wait()

    def block_of(source, target):
        def step(i, _):
            rows = pl.ds(i * 4, 4)
            parts = eliminate_rows(source[rows].reshape(512, 1024), lower, inverse_set.at[0])
            for k in range(4):
                target[rows, :, k * 256 : (k + 1) * 256] = parts[k].reshape(4, TILE, 256)
            return 0

        return step

    lax.fori_loop(0, 4, block_of(rows_v, rows_v), 0)
    table_copy = pltpu.make_async_copy(tab_v, tab_raw, lsem.at[20])
    table_copy.start()

    def wait_tile(t):
        push(theirs.at[t], t, 0, sibling).wait_recv()

    def forward(t):
        return push(theirs.at[t], t, t >> 1, sibling)

    for tiles in ((0, 2, 1, 3), (4, 6), (5, 7)):

        @pl.when(is_source)
        def _():
            for t in tiles:
                for copy in own_tiles(t, t + 1):
                    copy.wait()

        @pl.when(jnp.logical_not(on_source_chip))
        def _():
            for parity in (0, 1):
                mine = [t for t in tiles if t % 2 == parity]

                @pl.when(core == parity)
                def _():
                    for t in mine:
                        wait_tile(t)
                        forward(t).start()

            for parity in (0, 1):
                other = [t for t in tiles if t % 2 == parity]

                @pl.when(core != parity)
                def _():
                    for t in other:
                        wait_tile(t)

        @pl.when(on_source_chip & jnp.logical_not(is_source))
        def _():
            for t in tiles:
                wait_tile(t)

        joined = jnp.concatenate([theirs[t] for t in tiles], axis=0)
        parts = eliminate_rows(joined, lower, inverse_set.at[0])
        for i, t in enumerate(tiles):
            for k in range(4):
                theirs_e[t, :, k * 256 : (k + 1) * 256] = parts[k][i * TILE : (i + 1) * TILE]

    table_copy.wait()
    for r, (count, last) in enumerate(TABLE_ROWS):
        for at in range(count):
            tab[r, at] = within(tab_raw[r, at], last)
    for m in range(8):
        theirs_p[m] = theirs_e[tab[1, m]]
    for copy in load_contrib:
        copy.wait()

    def update(s):
        rows = slice(s * size, (s + 1) * size)
        for q in range(16):
            left[q] = rows_v[tab[0, q], rows]

        def two_cols(n, _):
            product = nt(
                left[...].reshape(16 * size, 1024), theirs_p[pl.ds(n * 2, 2)].reshape(256, 1024)
            )
            for t in range(2):
                for q in range(16):
                    tile = contrib_v[tab[1, 2 * n + t], tab[0, q], rows].astype(F32)
                    part = product[q * size : (q + 1) * size, t * TILE : (t + 1) * TILE]
                    packed[s, (q // 4) * 8 + 2 * n + t, q % 4] = (tile - part).astype(BF16)
            return 0

        lax.fori_loop(0, 4, two_cols, 0)

    def first_send(s):
        def send(t, _):
            _, row2, col2 = peer_of(front, z, core, x, (t * ORDER1) & 31)
            pltpu.make_async_remote_copy(
                src_ref=packed.at[s, row2 * 8 + col2], dst_ref=spread[s].at[here],
                send_sem=s1.at[s], recv_sem=r1.at[s],
                device_id=(front, row2, col2), device_id_type=MESH,
            ).start()
            return 0

        lax.fori_loop(1, 32, send, 0)
        spread[s][here] = packed[s, here]

    def first_all(s):
        return pltpu.make_async_remote_copy(
            src_ref=packed.at[s, pl.ds(0, 31)], dst_ref=spread[s].at[pl.ds(0, 31)],
            send_sem=s1.at[s], recv_sem=r1.at[s],
            device_id=(front, row, col), device_id_type=MESH,
        )

    def second_peer(t):
        return peer_of(front, z, core, x, (t * ORDER2) & 127)

    def second_copy(s, t):
        return pltpu.make_async_remote_copy(
            src_ref=ordered.at[s, t], dst_ref=landed[s].at[everywhere],
            send_sem=s2.at[s], recv_sem=r2.at[s],
            device_id=second_peer(t), device_id_type=MESH,
        )

    def second_send(s):
        def fill(t):
            f2, row2, col2 = second_peer(t)
            g = f2 * 4 + row2
            ordered[s, t] = spread[s][tab[2, g] + tab[3, col2], tab[6, g]]

        for t in range(GROUP):
            fill(t)
        landed[s][everywhere] = ordered[s, 0]
        for t in range(1, GROUP):
            second_copy(s, t).start()

        def step(i, _):
            for t in range(GROUP):
                fill(i * GROUP + t)
            for t in range(GROUP):
                second_copy(s, i * GROUP + t).start()
            return 0

        lax.fori_loop(1, 128 // GROUP, step, 0)

    def second_all(s):
        return pltpu.make_async_remote_copy(
            src_ref=ordered.at[s, pl.ds(0, 127)], dst_ref=landed[s].at[pl.ds(0, 127)],
            send_sem=s2.at[s], recv_sem=r2.at[s],
            device_id=(front, row, col), device_id_type=MESH,
        )

    def strip(a, s):
        return pl.ds(a * TILE + s * size, size)

    def write(a, s):
        return pltpu.make_async_copy(schur_v.at[strip(a, s)], schur.at[strip(a, s)], osem.at[s, a])

    def assemble(s):
        def row_of_tiles(a, _):
            rows = pl.ds(pl.multiple_of(a * TILE + s * size, size), size)
            for b in range(10):
                cols = slice(b * TILE, (b + 1) * TILE)
                total = init_v[rows, cols].astype(F32)
                for f in range(4):
                    m, k = tab[4, f * 5 + a], tab[5, f * 10 + b]
                    at = f * 32 + jnp.maximum(m - 1, 0) * 8 + jnp.maximum(k - 1, 0)
                    total = total + jnp.where((m > 0) & (k > 0), landed[s][at].astype(F32), 0.0)
                schur_v[rows, cols] = total
                rounded[pl.ds(pl.multiple_of(a * size, size), size), cols] = total.astype(BF16)
            return 0

        lax.fori_loop(0, 5, row_of_tiles, 0)
        for a in range(5):
            write(a, s).start()
        partial[s] = (
            jnp.dot(rounded[...], vectors_v[...], preferred_element_type=F32)
            .astype(BF16)
            .reshape(5, units, UNIT, partial.shape[-1])
        )

    def product_copies(s):
        copies = []
        for a in range(5):
            for j in range(units):
                u = (a * TILE + s * size) // UNIT + j
                copies.append(
                    (
                        u // 5,
                        u % 5,
                        partial.at[s, a, j],
                        pltpu.make_async_remote_copy(
                            src_ref=partial.at[s, a, j], dst_ref=sums.at[col, u % 5],
                            send_sem=s3, recv_sem=r3,
                            device_id=(front, row, u // 5), device_id_type=MESH,
                        ),
                    )
                )
        return copies

    def product_send(s):
        for to, at, value, copy in product_copies(s):

            @pl.when(col != to)
            def _():
                copy.start()

            @pl.when(col == to)
            def _():
                sums[to, at] = value[...]

    def product_all():
        return pltpu.make_async_remote_copy(
            src_ref=sums.at[pl.ds(0, 7)], dst_ref=sums.at[pl.ds(0, 7)], send_sem=s3, recv_sem=r3,
            device_id=(front, row, col), device_id_type=MESH,
        )

    for s in range(PARTS):
        update(s)
        first_send(s)
    for s in range(PARTS):
        first_all(s).wait_recv()
        second_send(s)
    load_init.wait()
    load_vectors.wait()
    for s in range(PARTS):
        second_all(s).wait_recv()
        assemble(s)
        product_send(s)
    for s in range(PARTS):
        first_all(s).wait_send()
        second_all(s).wait_send()
    product_all().wait_recv()
    total = sums[0].astype(F32)
    for c in range(1, 8):
        total = total + sums[c].astype(F32)
    product[...] = total.reshape(product.shape)
    product_all().wait_send()
    for s in range(PARTS):
        for a in range(5):
            write(a, s).wait()

    @pl.when(is_source)
    def _():
        for copy in source_sends():
            copy.wait_send()

    @pl.when(jnp.logical_not(on_source_chip))
    def _():
        for i in range(4):
            forward(2 * i + core).wait_send()


def fronts(row_tiles, col_tiles, owner, pivot, border, contrib, inverse_set, init, vectors):
    hbm = pl.BlockSpec(memory_space=pl.ANY)
    vmem = pl.BlockSpec(memory_space=pltpu.VMEM)
    size = TILE // PARTS
    rows, cols = init.shape
    wide = vectors.shape[1]
    return pl.pallas_call(
        front_kernel,
        out_shape=(
            jax.ShapeDtypeStruct((rows, cols), F32),
            jax.ShapeDtypeStruct((rows // 8, wide), F32),
        ),
        in_specs=[vmem, vmem, vmem, hbm, hbm, hbm, vmem, hbm, hbm],
        out_specs=(hbm, vmem),
        scratch_shapes=[
            pltpu.VMEM((8, TILE), jnp.int32),
            pltpu.SMEM((8, TILE), jnp.int32),
            pltpu.SMEM((8, TILE), jnp.int32),
            pltpu.VMEM((16, TILE, 1024), BF16),
            pltpu.VMEM((8, TILE, 1024), BF16),
            pltpu.VMEM((8, TILE, 1024), BF16),
            pltpu.VMEM((8, TILE, 1024), BF16),
            pltpu.VMEM((1024, 1024), BF16),
            pltpu.VMEM((8, 16, TILE, TILE), BF16),
            pltpu.VMEM((16, size, 1024), BF16),
            pltpu.VMEM((PARTS, 32, 4, size, TILE), BF16),
            pltpu.VMEM((PARTS, 128, size, TILE), BF16),
            pltpu.VMEM((rows, cols), BF16),
            pltpu.VMEM((cols, wide), BF16),
            pltpu.VMEM((rows, cols), F32),
            pltpu.VMEM((5 * size, cols), BF16),
            pltpu.VMEM((PARTS, 5, size // UNIT, UNIT, wide), BF16),
            pltpu.VMEM((8, 5, UNIT, wide), BF16),
            pltpu.SemaphoreType.DMA((16,)),
            pltpu.SemaphoreType.DMA((8,)),
            pltpu.SemaphoreType.DMA((21,)),
            *[pltpu.SemaphoreType.DMA((PARTS,))] * 4,
            pltpu.SemaphoreType.DMA((PARTS, 5)),
            pltpu.SemaphoreType.DMA,
            pltpu.SemaphoreType.DMA,
            *[pltpu.VMEM((32, 4, size, TILE), BF16)] * PARTS,
            *[pltpu.VMEM((128, size, TILE), BF16)] * PARTS,
        ],
        compiler_params=pltpu.CompilerParams(
            collective_id=0, has_side_effects=True, vmem_limit_bytes=60 << 20
        ),
        name="fronts",
    )(
        row_tiles, col_tiles, owner.reshape(1, owner.size), pivot, border.reshape(16, TILE, 1024),
        contrib.reshape(16, TILE, 1024), inverse_set, init, vectors,
    )


def shards(pivot_block, border, contrib, inverses, row_tiles, col_tiles, owner, schur_init, block):
    return fronts(
        row_tiles, col_tiles, owner, pivot_block, border, contrib, inverses, schur_init, block
    )


def solution(mesh):
    in_specs = (
        P("front", None, None),
        P("front", "row", None),
        P("front", "row", "col"),
        P("front", None, None, None),
        P(),
        P(),
        P(),
        P(("front", "row"), "col"),
        P("col", None),
    )
    out_specs = (P(("front", "row"), "col"), P(("front", "row", "col"), None))
    return jax.shard_map(shards, mesh=mesh, in_specs=in_specs, out_specs=out_specs, check_vma=False)
```
